32 devices in a mesh: dp: 2 (over x), sp: 16 (over z, y, core).
Axes of the slice: x: 2, y: 2, z: 4, core: 2. Of those that a mesh axis runs over, the one named last changes fastest.
Arguments:
- hidden: bfloat16 [128, 2816], P('dp'), parts along dimension 0
- ln_gamma: float32 [2816], replicated
- ln_beta: float32 [2816], replicated
- w_qkv: bfloat16 [2816, 3072], replicated
- w_out: bfloat16 [2816, 2816], replicated
- w_up: bfloat16 [2816, 11264], P(None, 'sp')
- w_down: bfloat16 [11264, 2816], P('sp')
- k_cache: bfloat16 [128, 8192, 128], P('dp', 'sp'), parts along dimension 0
- v_cache: bfloat16 [128, 8192, 128], P('dp', 'sp'), parts along dimension 0
- positions: int32 [128], P('dp'), parts along dimension 0
Outputs:
- output 1: bfloat16 [128, 2816], P('dp'), parts along dimension 0
- output 2: bfloat16 [128, 8192, 128], P('dp', 'sp'), parts along dimension 0
- output 3: bfloat16 [128, 8192, 128], P('dp', 'sp'), parts along dimension 0
There are 2 independent parts. The reference program is written for one: setup_inputs(seed, part) draws one part's arguments, and reference() takes and returns one part's arrays. A program takes and returns all parts, laid end to end along the dimension named above; an argument that names none is the same for every part.
All inputs are finite; a program needn't handle non-finite values.
Results may differ from the reference program's by a relative error of at most 0.00633762.
Values sent between devices are 32-bit elements.
A program may use at most 1 GiB of HBM per device.

```python
import jax
import jax.numpy as jnp
from jax import lax

BATCH_ROWS = 64
D_MODEL = 2816
N_HEADS = 22
HEAD_DIM = 128
FF_DIM = 11264
SEQ_SHARD = 512
N_SHARDS = 16
SEQ_LEN = N_SHARDS * SEQ_SHARD
LN_EPS = 1e-5
ROPE_BASE = 10000.0
NEG_FILL = -1e30


def setup_inputs(seed: int = 0, part: int = 0) -> dict:
    base_key = jax.random.key(seed)
    weight_keys = jax.random.split(base_key, 6)
    part_keys = jax.random.split(jax.random.fold_in(base_key, part), 4)
    hidden = jax.random.normal(part_keys[0], (BATCH_ROWS, D_MODEL), jnp.float32).astype(jnp.bfloat16)
    ln_gamma = 1.0 + 0.3 * jax.random.normal(weight_keys[0], (D_MODEL,), jnp.float32)
    ln_beta = 0.3 * jax.random.normal(weight_keys[1], (D_MODEL,), jnp.float32)
    w_qkv = (jax.random.normal(weight_keys[2], (D_MODEL, (N_HEADS + 2) * HEAD_DIM), jnp.float32) * D_MODEL ** -0.5).astype(jnp.bfloat16)
    out_scale = 0.5 * SEQ_LEN ** 0.5 * (N_HEADS * HEAD_DIM) ** -0.5
    w_out = (jax.random.normal(weight_keys[3], (N_HEADS * HEAD_DIM, D_MODEL), jnp.float32) * out_scale).astype(jnp.bfloat16)
    w_up = (jax.random.normal(weight_keys[4], (D_MODEL, FF_DIM), jnp.float32) * D_MODEL ** -0.5).astype(jnp.bfloat16)
    w_down = (jax.random.normal(weight_keys[5], (FF_DIM, D_MODEL), jnp.float32) * FF_DIM ** -0.5).astype(jnp.bfloat16)
    k_cache = jax.random.normal(part_keys[1], (BATCH_ROWS, SEQ_LEN, HEAD_DIM), jnp.float32).astype(jnp.bfloat16)
    v_cache = jax.random.normal(part_keys[2], (BATCH_ROWS, SEQ_LEN, HEAD_DIM), jnp.float32).astype(jnp.bfloat16)
    positions = jax.random.randint(part_keys[3], (BATCH_ROWS,), SEQ_LEN // 2, SEQ_LEN, dtype=jnp.int32)
    positions = positions.at[0].set(SEQ_LEN - 1).at[1].set(SEQ_LEN // 2)
    return {'hidden': hidden, 'ln_gamma': ln_gamma, 'ln_beta': ln_beta, 'w_qkv': w_qkv, 'w_out': w_out, 'w_up': w_up, 'w_down': w_down, 'k_cache': k_cache, 'v_cache': v_cache, 'positions': positions}


def layer_norm(hidden, ln_gamma, ln_beta):
    hidden_f32 = hidden.astype(jnp.float32)
    row_mean = jnp.mean(hidden_f32, axis=-1, keepdims=True)
    centered = hidden_f32 - row_mean
    row_var = jnp.mean(centered * centered, axis=-1, keepdims=True)
    return (centered * lax.rsqrt(row_var + LN_EPS) * ln_gamma + ln_beta).astype(jnp.bfloat16)


def rotary_tables(positions, head_dim):
    inv_freq = 1.0 / (ROPE_BASE ** (jnp.arange(0, head_dim, 2, dtype=jnp.float32) / head_dim))
    angles = positions.astype(jnp.float32)[:, None] * inv_freq[None, :]
    cos_half = jnp.cos(angles)
    sin_half = jnp.sin(angles)
    return jnp.concatenate([cos_half, cos_half], axis=-1), jnp.concatenate([sin_half, sin_half], axis=-1)


def apply_rotary(vecs, cos_full, sin_full):
    vecs_f32 = vecs.astype(jnp.float32)
    half_dim = vecs.shape[-1] // 2
    rotated = jnp.concatenate([-vecs_f32[..., half_dim:], vecs_f32[..., :half_dim]], axis=-1)
    return (vecs_f32 * cos_full + rotated * sin_full).astype(jnp.bfloat16)


def row_attention(row_inputs):
    q_row, k_row, v_row, pos_row = row_inputs
    scores = jnp.dot(q_row, k_row.T, preferred_element_type=jnp.float32) * HEAD_DIM ** -0.5
    scores = scores.reshape(N_HEADS, N_SHARDS, SEQ_SHARD)
    valid_mask = (jnp.arange(SEQ_LEN) <= pos_row).reshape(N_SHARDS, SEQ_SHARD)
    masked = jnp.where(valid_mask, scores, NEG_FILL)
    block_max = jnp.max(masked, axis=-1)
    exp_scores = jnp.where(valid_mask, jnp.exp(masked - block_max[..., None]), 0.0)
    block_sum = jnp.sum(exp_scores, axis=-1)
    block_ctx = jnp.einsum('hcs,csd->hcd', exp_scores.astype(jnp.bfloat16).astype(jnp.float32), v_row.reshape(N_SHARDS, SEQ_SHARD, HEAD_DIM).astype(jnp.float32))
    top_max = jnp.max(block_max, axis=-1)
    scale_w = jnp.exp(block_max - top_max[:, None])
    total_sum = jnp.sum(block_sum * scale_w, axis=-1)
    total_ctx = jnp.sum(block_ctx * scale_w[..., None], axis=1)
    return (total_ctx / total_sum[:, None]).astype(jnp.bfloat16)


def reference(hidden, ln_gamma, ln_beta, w_qkv, w_out, w_up, w_down, k_cache, v_cache, positions):
    normed = layer_norm(hidden, ln_gamma, ln_beta)
    qkv_proj = jnp.dot(normed, w_qkv, preferred_element_type=jnp.float32).astype(jnp.bfloat16)
    qkv_proj = qkv_proj.reshape(BATCH_ROWS, N_HEADS + 2, HEAD_DIM)
    cos_full, sin_full = rotary_tables(positions, HEAD_DIM)
    q_rot = apply_rotary(qkv_proj[:, :N_HEADS], cos_full[:, None, :], sin_full[:, None, :])
    k_rot = apply_rotary(qkv_proj[:, N_HEADS], cos_full, sin_full)
    v_new = qkv_proj[:, N_HEADS + 1]
    write_mask = (jnp.arange(SEQ_LEN)[None, :] == positions[:, None])[:, :, None]
    k_next = jnp.where(write_mask, k_rot[:, None, :], k_cache)
    v_next = jnp.where(write_mask, v_new[:, None, :], v_cache)
    context = lax.map(row_attention, (q_rot, k_next, v_next, positions))
    attn_out = jnp.dot(context.reshape(BATCH_ROWS, N_HEADS * HEAD_DIM), w_out, preferred_element_type=jnp.float32)
    up_proj = jnp.dot(normed, w_up, preferred_element_type=jnp.float32)
    activated = jax.nn.gelu(up_proj, approximate=False).astype(jnp.bfloat16)
    mlp_out = jnp.dot(activated, w_down, preferred_element_type=jnp.float32)
    out_hidden = (hidden.astype(jnp.float32) + attn_out + mlp_out).astype(jnp.bfloat16)
    return (out_hidden, k_next, v_next)
```

```python
import functools
import math

import jax
import jax.numpy as jnp
from jax import lax
from jax.experimental import pallas as pl
from jax.experimental.pallas import tpu as pltpu
from jax.sharding import PartitionSpec as P

LN_EPS = 1e-5
ROPE_BASE = 10000.0
NEG_FILL = -1e30
MESH = pl.DeviceIdType.MESH

ROWS = 64
D = 2816
HD = 128
NH = 22
HALF = 11
FF = 704
SEQ = 512
GROUPS = 8
LANE_L = 64
QCHUNK = 512
NQ = 6
QSLOTS = 4
F32 = jnp.float32
BF16 = jnp.bfloat16


def rope(vec, cos, sin_signed):
    return (vec * cos + pltpu.roll(vec, HD // 2, 1) * sin_signed).astype(BF16).astype(F32)


def remote(src, dst, ssem, rsem, dev):
    return pltpu.make_async_remote_copy(src, dst, ssem, rsem, device_id=dev, device_id_type=MESH)


def weights_of(tile, top):
    return jnp.exp(tile - top)


def main_kernel(pos, x_ref, g_ref, b_ref, cos_ref, sin_ref, wqkv, wout, wup, wdn, kh, vh,
                agb, ko, vo,
                wq, wu, wd, h_s, act, q4, kn, vn,
                st, d2d, cmb, rcv, ml, mld, mls, mly, mlz, mlr, wsend, wrecv,
                qsem, osem, ksem, vsem,
                d2d_s, d2d_r, a2a_s, a2a_r, mld_s, mld_r, mly_s, mly_r, mlz_s, mlz_r, wo_s, wo_r,
                agz_s, agz_r, agy_s, agy_r, agc_s, agc_r):
    dp = lax.axis_index("dp")
    me = lax.axis_index("sp")
    core = me % 2
    chip = me // 2
    y = chip % 2
    z = chip // 2
    partner = (dp, me + 1 - 2 * core)
    ypeer = (dp, me + 2 - 4 * y)

    def zpeer(d):
        return (dp, ((z + d) % 4) * 4 + y * 2 + core)

    def cpeer(d):
        return (dp, ((chip + d) % 8) * 2 + core)

    c_q = [pltpu.make_async_copy(wqkv.at[:, pl.ds(QCHUNK * i, QCHUNK)], wq.at[i % QSLOTS], qsem.at[i]) for i in range(NQ)]

    def c_kv(s):
        rows = pl.ds(8 * ((chip + s + 1) % 8), 8)
        return (pltpu.make_async_copy(kh.at[rows], ko.at[rows], ksem.at[s]),
                pltpu.make_async_copy(vh.at[rows], vo.at[rows], vsem.at[s]))

    def start_kv(s):
        for c in c_kv(s):
            c.start()

    c_o = [pltpu.make_async_copy(wout.at[pl.ds((2 * core + i) * FF, FF)], (wu, wd)[i], osem.at[i]) for i in range(2)]

    for i in range(QSLOTS):
        c_q[i].start()

    barrier = pltpu.get_barrier_semaphore()
    pl.semaphore_signal(barrier, inc=1, device_id=partner, device_id_type=MESH)
    for d in range(1, GROUPS):
        pl.semaphore_signal(barrier, inc=1, device_id=cpeer(d), device_id_type=MESH)

    def norm_rows(i, carry):
        rows = pl.ds(pl.multiple_of(16 * i, 16), 16)
        xf = x_ref[rows, :].astype(F32)
        cen = xf - jnp.mean(xf, axis=-1, keepdims=True)
        var = jnp.mean(cen * cen, axis=-1, keepdims=True)
        h_s[rows, :] = (cen * lax.rsqrt(var + LN_EPS) * g_ref[...] + b_ref[...]).astype(BF16)
        return carry

    lax.fori_loop(0, ROWS // 16, norm_rows, 0)

    up = lax.dot_general(h_s[...], wup[...], (((1,), (1,)), ((), ())), preferred_element_type=F32)
    act[...] = (0.5 * up * (1.0 + lax.erf(up * (1.0 / math.sqrt(2.0))))).astype(BF16)
    for n in range(HALF):
        part = jnp.dot(act[...], wdn[:, 256 * n:256 * (n + 1)], preferred_element_type=F32)
        for j in (2 * n, 2 * n + 1):
            ml[:, j // HALF, j % HALF] = part[:, 128 * (j - 2 * n):128 * (j - 2 * n + 1)].reshape(GROUPS, 8, HD)
    pl.semaphore_wait(barrier, GROUPS)
    r_mld = remote(ml.at[:, 1 - core], mld, mld_s, mld_r, partner)
    r_mld.start()

    cos = cos_ref[...]
    sin = sin_ref[...]
    r_mly = remote(mls.at[:, 1 - y], mly, mly_s, mly_r, ypeer)
    for ch in range(NQ):
        c_q[ch].wait()
        acc = jnp.dot(h_s[...], wq[ch % QSLOTS], preferred_element_type=F32).astype(BF16).astype(F32)
        if ch + QSLOTS < NQ:
            c_q[ch + QSLOTS].start()
        if ch >= 2:
            start_kv(ch - 2)
        for i in range(QCHUNK // HD):
            h = ch * (QCHUNK // HD) + i
            vec = acc[:, HD * i:HD * (i + 1)]
            if h <= NH:
                vec = rope(vec, cos, sin)
            vec = vec.reshape(GROUPS, 8, HD)
            if h < NH:
                q4[:, h] = vec
            elif h == NH:
                kn[...] = vec
            else:
                vn[...] = vec
        if ch == 2:
            r_mld.wait_recv()
            mls[...] = ml[:, core].reshape(4, 2, HALF, 8, HD) + mld[...].reshape(4, 2, HALF, 8, HD)
            r_mly.start()

    row_id = lax.broadcasted_iota(jnp.int32, (SEQ, HD), 0)
    col_id = lax.broadcasted_iota(jnp.int32, (NH, SEQ), 1)
    sub = lax.broadcasted_iota(jnp.int32, (NH, HD), 0)
    lane = lax.broadcasted_iota(jnp.int32, (NH, HD), 1)

    def attend(s):
        p = (chip + s + 1) % 8
        for r in range(8):
            b = 8 * p + r
            local = pos[b] - me * SEQ
            here = row_id == local
            kb = jnp.where(here, jnp.broadcast_to(kn[p, r:r + 1, :], (SEQ, HD)).astype(BF16), ko[b])
            vb = jnp.where(here, jnp.broadcast_to(vn[p, r:r + 1, :], (SEQ, HD)).astype(BF16), vo[b])
            ko[b] = kb
            vo[b] = vb
            q = q4[p, :, r, :].astype(BF16)
            sc = lax.dot_general(q, kb, (((1,), (1,)), ((), ())), preferred_element_type=F32) * HD ** -0.5
            valid = col_id <= local
            sc = jnp.where(valid, sc, NEG_FILL)
            m = jnp.max(sc, axis=-1, keepdims=True)
            e = jnp.where(valid, jnp.exp(sc - m), 0.0)
            l = jnp.sum(e, axis=-1, keepdims=True)
            o = jnp.dot(e.astype(BF16), vb, preferred_element_type=F32)
            for half in range(2):
                idx = sub - HALF * half
                own = (idx >= 0) & (idx < HALF)
                t = jnp.where(own & (lane == idx), m, jnp.where(own & (lane == idx + LANE_L), l, 0.0))
                st[s, half, HALF, r:r + 1, :] = jnp.sum(t, axis=0, keepdims=True)
                st[s, half, 0:HALF, r, :] = o[HALF * half:HALF * (half + 1), :]

    def r_d2d(s):
        return remote(st.at[s, 1 - core], d2d.at[s], d2d_s.at[s], d2d_r.at[s], partner)

    def r_a2a(s):
        return remote(cmb.at[s], rcv.at[s], a2a_s.at[s], a2a_r.at[s], cpeer(s + 1))

    lane8 = lax.broadcasted_iota(jnp.int32, (8, HD), 1)

    def pair(s):
        r_d2d(s).wait_recv()
        ta, tb = st[s, core, HALF], d2d[s, HALF]
        top = jnp.maximum(ta, tb)
        wa, wb = weights_of(ta, top), weights_of(tb, top)
        total = ta * pltpu.roll(wa, LANE_L, 1) + tb * pltpu.roll(wb, LANE_L, 1)
        cmb[s, HALF] = jnp.where(lane8 < LANE_L, top, total)
        for i in range(HALF):
            cmb[s, i] = st[s, core, i] * wa[:, i:i + 1] + d2d[s, i] * wb[:, i:i + 1]

    r_mlz = [remote(mlz.at[(z + d) % 4], mlr.at[d - 1], mlz_s.at[d - 1], mlz_r.at[d - 1], zpeer(d)) for d in range(1, 4)]

    def step(s, carry):
        ck, cv = c_kv(s)
        ck.wait()
        cv.wait()

        @pl.when(s < 4)
        def _():
            start_kv(s + 4)

        @pl.when(s == 4)
        def _():
            c_o[0].start()

        @pl.when(s == 5)
        def _():
            c_o[1].start()

        @pl.when(s == 1)
        def _():
            r_mly.wait_recv()
            mlz[...] = mls[:, y] + mly[...]
            for c in r_mlz:
                c.start()

        attend(s)
        r_d2d(s).start()

        @pl.when(s > 0)
        def _():
            pair(s - 1)
            r_a2a(s - 1).start()

        return carry

    lax.fori_loop(0, GROUPS, step, 0)
    pair(GROUPS - 1)

    for c in r_mlz:
        c.wait_recv()
    fin = mlz[z] + mlr[0] + mlr[1] + mlr[2]

    for s in range(GROUPS - 1):
        r_a2a(s).wait_recv()
    tiles = [cmb[GROUPS - 1, HALF]] + [rcv[s, HALF] for s in range(GROUPS - 1)]
    top = functools.reduce(jnp.maximum, tiles)
    ws = [weights_of(t, top) for t in tiles]
    total = functools.reduce(jnp.add, [t * pltpu.roll(w, LANE_L, 1) for t, w in zip(tiles, ws)])
    heads = []
    for i in range(HALF):
        acc = cmb[GROUPS - 1, i] * ws[0][:, i:i + 1]
        for s in range(GROUPS - 1):
            acc += rcv[s, i] * ws[s + 1][:, i:i + 1]
        heads.append((acc / total[:, LANE_L + i:LANE_L + i + 1]).astype(BF16))
    ctx = jnp.concatenate(heads, axis=1)

    def project(column_half):
        cols = pl.ds(pl.multiple_of(HALF * HD * column_half, HD), HALF * HD)
        return (jnp.dot(ctx[:, :FF], wu[:, cols], preferred_element_type=F32)
                + jnp.dot(ctx[:, FF:], wd[:, cols], preferred_element_type=F32))

    c_o[0].wait()
    c_o[1].wait()
    other = project(1 - core)
    for i in range(HALF):
        wsend[i] = other[:, HD * i:HD * (i + 1)]
    r_wo = remote(wsend, wrecv, wo_s, wo_r, partner)
    r_wo.start()
    mine = project(core)
    r_wo.wait_recv()
    for i in range(HALF):
        agb[chip, core, i] = mine[:, HD * i:HD * (i + 1)] + wrecv[i] + fin[i]

    def piece(zz, yy):
        return agb.at[zz * 2 + yy, core]

    def send_z(d):
        return remote(piece(z, y), piece(z, y), agz_s.at[d - 1], agz_r.at[d - 1], zpeer(d))

    def send_y(d):
        zz = (z + 4 - d) % 4
        return remote(piece(zz, y), piece(zz, y), agy_s.at[d], agy_r.at[d], ypeer)

    def send_c(d, other_y):
        zz = (z + 4 - d) % 4
        yy = (y + other_y) % 2
        return remote(piece(zz, yy), piece(zz, yy), agc_s.at[2 * d + other_y], agc_r.at[2 * d + other_y], partner)

    for d in (2, 1, 3):
        send_z(d).start()
    send_y(0).start()
    send_c(0, 0).start()
    for d in (1, 2, 3):
        send_z(d).wait_recv()
        send_y(d).start()
        send_c(d, 0).start()
    for d in range(4):
        send_y(d).wait_recv()
        send_c(d, 1).start()
    for d in range(4):
        for o in range(2):
            send_c(d, o).wait_recv()

    r_mld.wait_send()
    r_mly.wait_send()
    for c in r_mlz:
        c.wait_send()
    for s in range(GROUPS):
        r_d2d(s).wait_send()
    for s in range(GROUPS - 1):
        r_a2a(s).wait_send()
    r_wo.wait_send()
    for d in (1, 2, 3):
        send_z(d).wait_send()
    for d in range(4):
        send_y(d).wait_send()
        send_c(d, 0).wait_send()
        send_c(d, 1).wait_send()


def write_kernel(ko, vo, agb, x_ref, out_ref, k_out, v_out, sem):
    copies = []
    for i in range(8):
        rows = pl.ds(8 * i, 8)
        copies.append(pltpu.make_async_copy(ko.at[rows], k_out.at[rows], sem.at[2 * i]))
        copies.append(pltpu.make_async_copy(vo.at[rows], v_out.at[rows], sem.at[2 * i + 1]))
    for c in copies:
        c.start()
    for q in range(GROUPS // 2):
        rows = slice(16 * q, 16 * (q + 1))
        for j in range(NH):
            cols = slice(HD * j, HD * (j + 1))
            both = agb[2 * q:2 * q + 2, j // HALF, j % HALF].reshape(16, HD)
            out_ref[rows, cols] = (x_ref[rows, cols].astype(F32) + both).astype(BF16)
    for c in copies:
        c.wait()


def device_step(hidden, ln_gamma, ln_beta, w_qkv, w_out, w_up, w_down, k_cache, v_cache, positions):
    inv_freq = 1.0 / (ROPE_BASE ** (jnp.arange(0, HD, 2, dtype=F32) / HD))
    angles = positions.astype(F32)[:, None] * inv_freq[None, :]
    cos, sin = jnp.cos(angles), jnp.sin(angles)
    cos_full = jnp.concatenate([cos, cos], axis=-1)
    sin_signed = jnp.concatenate([-sin, sin], axis=-1)

    vmem = pl.BlockSpec(memory_space=pltpu.VMEM)
    hbm = pl.BlockSpec(memory_space=pltpu.HBM)
    smem = pl.BlockSpec(memory_space=pltpu.SMEM)
    dma = pltpu.SemaphoreType.DMA
    agb, k_new, v_new = pl.pallas_call(
        main_kernel,
        out_shape=(
            jax.ShapeDtypeStruct((GROUPS, 2, HALF, 8, HD), F32),
            jax.ShapeDtypeStruct(k_cache.shape, BF16),
            jax.ShapeDtypeStruct(v_cache.shape, BF16),
        ),
        in_specs=[smem] + [vmem] * 5 + [hbm] * 2 + [vmem] * 2 + [hbm] * 2,
        out_specs=(vmem, vmem, vmem),
        scratch_shapes=[
            pltpu.VMEM((QSLOTS, D, QCHUNK), BF16),
            pltpu.VMEM((FF, D), BF16),
            pltpu.VMEM((FF, D), BF16),
            pltpu.VMEM((ROWS, D), BF16),
            pltpu.VMEM((ROWS, FF), BF16),
            pltpu.VMEM((GROUPS, NH, 8, HD), F32),
            pltpu.VMEM((GROUPS, 8, HD), F32),
            pltpu.VMEM((GROUPS, 8, HD), F32),
            pltpu.VMEM((GROUPS, 2, HALF + 1, 8, HD), F32),
            pltpu.VMEM((GROUPS, HALF + 1, 8, HD), F32),
            pltpu.VMEM((GROUPS, HALF + 1, 8, HD), F32),
            pltpu.VMEM((GROUPS - 1, HALF + 1, 8, HD), F32),
            pltpu.VMEM((GROUPS, 2, HALF, 8, HD), F32),
            pltpu.VMEM((GROUPS, HALF, 8, HD), F32),
            pltpu.VMEM((4, 2, HALF, 8, HD), F32),
            pltpu.VMEM((4, HALF, 8, HD), F32),
            pltpu.VMEM((4, HALF, 8, HD), F32),
            pltpu.VMEM((3, HALF, 8, HD), F32),
            pltpu.VMEM((HALF, 8, HD), F32),
            pltpu.VMEM((HALF, 8, HD), F32),
            dma((NQ,)), dma((2,)), dma((GROUPS,)), dma((GROUPS,)),
            dma((GROUPS,)), dma((GROUPS,)), dma((GROUPS - 1,)), dma((GROUPS - 1,)),
            dma, dma, dma, dma, dma((3,)), dma((3,)), dma, dma,
            dma((3,)), dma((3,)), dma((4,)), dma((4,)), dma((8,)), dma((8,)),
        ],
        compiler_params=pltpu.CompilerParams(collective_id=0, has_side_effects=True, vmem_limit_bytes=28 * 2**20),
        name="layer",
    )(positions, hidden, ln_gamma.reshape(1, D), ln_beta.reshape(1, D), cos_full, sin_signed,
      w_qkv, w_out, w_up.T, w_down, k_cache, v_cache)

    return pl.pallas_call(
        write_kernel,
        out_shape=(
            jax.ShapeDtypeStruct(hidden.shape, BF16),
            jax.ShapeDtypeStruct(k_cache.shape, BF16),
            jax.ShapeDtypeStruct(v_cache.shape, BF16),
        ),
        in_specs=[vmem] * 4,
        out_specs=(vmem, hbm, hbm),
        scratch_shapes=[dma((16,))],
        compiler_params=pltpu.CompilerParams(vmem_limit_bytes=16 * 2**20),
        name="write",
    )(k_new, v_new, agb, hidden)


def solution(mesh):
    cache_spec = P('dp', 'sp', None)
    in_specs = (P('dp', None), P(None), P(None), P(None, None), P(None, None), P(None, 'sp'), P('sp', None), cache_spec, cache_spec, P('dp'))
    out_specs = (P('dp', None), cache_spec, cache_spec)
    return jax.shard_map(device_step, mesh=mesh, in_specs=in_specs, out_specs=out_specs, check_vma=False)
```

```python
import functools
import math

import jax
import jax.numpy as jnp
import numpy as np
from jax import lax
from jax.experimental import pallas as pl
from jax.experimental.pallas import tpu as pltpu
from jax.sharding import PartitionSpec as P

LN_EPS = 1e-5
ROPE_BASE = 10000.0
NEG_FILL = -1e30
MESH = pl.DeviceIdType.MESH

ROWS = 64
D = 2816
HD = 128
NH = 22
HALF = 11
FF = 704
SEQ = 512
GROUPS = 8
LANE_L = 64
QCHUNK = 512
NQ = 6
QSLOTS = 4
F32 = jnp.float32
BF16 = jnp.bfloat16


def rope(vec, cos, sin_signed):
    return (vec * cos + pltpu.roll(vec, HD // 2, 1) * sin_signed).astype(BF16).astype(F32)


def remote(src, dst, ssem, rsem, dev):
    return pltpu.make_async_remote_copy(src, dst, ssem, rsem, device_id=dev, device_id_type=MESH)


def weights_of(tile, top):
    return jnp.exp(tile - top)


def main_kernel(pos_h, x_h, g_h, b_h, freq_h, wqkv, wout, wup, wdn, kh, vh,
                agb, ko, vo, kn, vn,
                pos, x_s, g_s, b_s, freq_s, posv, wq, wu, wd, h_s, act, q4,
                st, d2d, cmb, rcv, ml, mld, mls, mly, mlz, mlr, wsend, wrecv,
                isem, wsem, qsem, osem, ksem, vsem,
                d2d_s, d2d_r, a2a_s, a2a_r, mld_s, mld_r, mly_s, mly_r, mlz_s, mlz_r, wo_s, wo_r,
                agz_s, agz_r, agy_s, agy_r, agc_s, agc_r):
    dp = lax.axis_index("dp")
    me = lax.axis_index("sp")
    core = me % 2
    chip = me // 2
    y = chip % 2
    z = chip // 2
    partner = (dp, me + 1 - 2 * core)
    ypeer = (dp, me + 2 - 4 * y)

    def zpeer(d):
        return (dp, ((z + d) % 4) * 4 + y * 2 + core)

    def cpeer(d):
        return (dp, ((chip + d) % 8) * 2 + core)

    c_in = [pltpu.make_async_copy(src, dst, isem.at[i])
            for i, (src, dst) in enumerate(((x_h, x_s), (g_h, g_s), (b_h, b_s), (freq_h, freq_s), (pos_h, pos)))]
    c_up = pltpu.make_async_copy(wup, wu, wsem.at[0])
    c_dn = pltpu.make_async_copy(wdn, wd, wsem.at[1])
    c_q = [pltpu.make_async_copy(wqkv.at[:, pl.ds(QCHUNK * i, QCHUNK)], wq.at[i % QSLOTS], qsem.at[i]) for i in range(NQ)]

    def c_kv(s):
        rows = pl.ds(8 * ((chip + s + 1) % 8), 8)
        return (pltpu.make_async_copy(kh.at[rows], ko.at[rows], ksem.at[s]),
                pltpu.make_async_copy(vh.at[rows], vo.at[rows], vsem.at[s]))

    def start_kv(s):
        for c in c_kv(s):
            c.start()

    c_o = [pltpu.make_async_copy(wout.at[pl.ds((2 * core + i) * FF, FF)], (wu, wd)[i], osem.at[i]) for i in range(2)]

    for c in c_in + [c_up, c_dn]:
        c.start()
    for i in range(3):
        c_q[i].start()

    barrier = pltpu.get_barrier_semaphore()
    pl.semaphore_signal(barrier, inc=1, device_id=partner, device_id_type=MESH)
    for d in range(1, GROUPS):
        pl.semaphore_signal(barrier, inc=1, device_id=cpeer(d), device_id_type=MESH)

    for c in c_in:
        c.wait()
    gamma = g_s[...].reshape(1, D)
    beta = b_s[...].reshape(1, D)

    def norm_rows(i, carry):
        rows = pl.ds(pl.multiple_of(16 * i, 16), 16)
        xf = x_s[rows, :].astype(F32)
        cen = xf - jnp.mean(xf, axis=-1, keepdims=True)
        var = jnp.mean(cen * cen, axis=-1, keepdims=True)
        h_s[rows, :] = (cen * lax.rsqrt(var + LN_EPS) * gamma + beta).astype(BF16)
        return carry

    lax.fori_loop(0, ROWS // 16, norm_rows, 0)

    for b in range(ROWS):
        posv[b:b + 1, :] = jnp.full((1, HD), pos[b], jnp.int32)
    angles = posv[...].astype(F32) * freq_s[...]
    cos = jnp.cos(angles)
    sin = jnp.sin(angles)
    sin = jnp.where(lax.broadcasted_iota(jnp.int32, (ROWS, HD), 1) < HD // 2, -sin, sin)

    c_up.wait()
    c_q[3].start()
    up = lax.dot_general(h_s[...], wu[...], (((1,), (1,)), ((), ())), preferred_element_type=F32)
    act[...] = (0.5 * up * (1.0 + lax.erf(up * (1.0 / math.sqrt(2.0))))).astype(BF16)
    c_dn.wait()
    for n in range(HALF):
        part = jnp.dot(act[...], wd[:, 256 * n:256 * (n + 1)], preferred_element_type=F32)
        for j in (2 * n, 2 * n + 1):
            ml[:, j // HALF, j % HALF] = part[:, 128 * (j - 2 * n):128 * (j - 2 * n + 1)].reshape(GROUPS, 8, HD)
    pl.semaphore_wait(barrier, GROUPS)
    r_mld = remote(ml.at[:, 1 - core], mld, mld_s, mld_r, partner)
    r_mld.start()

    r_mly = remote(mls.at[:, 1 - y], mly, mly_s, mly_r, ypeer)
    for ch in range(NQ):
        c_q[ch].wait()
        acc = jnp.dot(h_s[...], wq[ch % QSLOTS], preferred_element_type=F32).astype(BF16).astype(F32)
        if ch + QSLOTS < NQ:
            c_q[ch + QSLOTS].start()
        if ch >= 2:
            start_kv(ch - 2)
        for i in range(QCHUNK // HD):
            h = ch * (QCHUNK // HD) + i
            vec = acc[:, HD * i:HD * (i + 1)]
            if h <= NH:
                vec = rope(vec, cos, sin)
            vec = vec.reshape(GROUPS, 8, HD)
            if h < NH:
                q4[:, h] = vec
            elif h == NH:
                kn[...] = vec
            else:
                vn[...] = vec
        if ch == 2:
            r_mld.wait_recv()
            mls[...] = ml[:, core].reshape(4, 2, HALF, 8, HD) + mld[...].reshape(4, 2, HALF, 8, HD)
            r_mly.start()

    col_id = lax.broadcasted_iota(jnp.int32, (NH, SEQ), 1)
    sub = lax.broadcasted_iota(jnp.int32, (NH, HD), 0)
    lane = lax.broadcasted_iota(jnp.int32, (NH, HD), 1)

    def attend(s):
        p = (chip + s + 1) % 8
        local = [pos[8 * p + r] - me * SEQ for r in range(8)]
        inside = [(x >= 0) & (x < SEQ) for x in local]
        qs = [q4[p, :, r, :] for r in range(8)]
        scores = [lax.dot_general(qs[r].astype(BF16), ko[8 * p + r], (((1,), (1,)), ((), ())), preferred_element_type=F32)
                  for r in range(8)]
        s_new = [jnp.sum(qs[r] * kn[p, r:r + 1, :], axis=-1, keepdims=True) * HD ** -0.5 for r in range(8)]
        s_new = [jnp.where(inside[r], s_new[r], NEG_FILL) for r in range(8)]
        masked = [jnp.where(col_id < local[r], scores[r] * HD ** -0.5, NEG_FILL) for r in range(8)]
        ms = [jnp.maximum(jnp.max(masked[r], axis=-1, keepdims=True), s_new[r]) for r in range(8)]
        es = [jnp.where(col_id < local[r], jnp.exp(masked[r] - ms[r]), 0.0) for r in range(8)]
        e_new = [jnp.where(inside[r], jnp.exp(s_new[r] - ms[r]), 0.0) for r in range(8)]
        os = [jnp.dot(es[r].astype(BF16), vo[8 * p + r], preferred_element_type=F32) for r in range(8)]
        ls = [jnp.sum(es[r], axis=-1, keepdims=True) + e_new[r] for r in range(8)]
        for r in range(8):
            o = os[r] + e_new[r].astype(BF16).astype(F32) * vn[p, r:r + 1, :]
            for half in range(2):
                idx = sub - HALF * half
                own = (idx >= 0) & (idx < HALF)
                t = jnp.where(own & (lane == idx), ms[r], jnp.where(own & (lane == idx + LANE_L), ls[r], 0.0))
                st[s, half, HALF, r:r + 1, :] = jnp.sum(t, axis=0, keepdims=True)
                st[s, half, 0:HALF, r, :] = o[HALF * half:HALF * (half + 1), :]

    def r_d2d(s):
        return remote(st.at[s, 1 - core], d2d.at[s], d2d_s.at[s], d2d_r.at[s], partner)

    def r_a2a(s):
        return remote(cmb.at[s], rcv.at[s], a2a_s.at[s], a2a_r.at[s], cpeer(s + 1))

    lane8 = lax.broadcasted_iota(jnp.int32, (8, HD), 1)

    def pair(s):
        r_d2d(s).wait_recv()
        ta, tb = st[s, core, HALF], d2d[s, HALF]
        top = jnp.maximum(ta, tb)
        wa, wb = weights_of(ta, top), weights_of(tb, top)
        total = ta * pltpu.roll(wa, LANE_L, 1) + tb * pltpu.roll(wb, LANE_L, 1)
        cmb[s, HALF] = jnp.where(lane8 < LANE_L, top, total)
        for i in range(HALF):
            cmb[s, i] = st[s, core, i] * wa[:, i:i + 1] + d2d[s, i] * wb[:, i:i + 1]

    r_mlz = [remote(mlz.at[(z + d) % 4], mlr.at[d - 1], mlz_s.at[d - 1], mlz_r.at[d - 1], zpeer(d)) for d in range(1, 4)]

    def step(s, carry):
        ck, cv = c_kv(s)
        ck.wait()
        cv.wait()

        @pl.when(s < 4)
        def _():
            start_kv(s + 4)

        @pl.when(s == 4)
        def _():
            c_o[0].start()

        @pl.when(s == 5)
        def _():
            c_o[1].start()

        @pl.when(s == 4)
        def _():
            r_mly.wait_recv()
            mlz[...] = mls[:, y] + mly[...]
            for c in r_mlz:
                c.start()

        attend(s)
        r_d2d(s).start()

        @pl.when(s > 0)
        def _():
            pair(s - 1)
            r_a2a(s - 1).start()

        return carry

    lax.fori_loop(0, GROUPS, step, 0)
    pair(GROUPS - 1)

    for c in r_mlz:
        c.wait_recv()
    fin = mlz[z] + mlr[0] + mlr[1] + mlr[2]

    for s in range(GROUPS - 1):
        r_a2a(s).wait_recv()
    tiles = [cmb[GROUPS - 1, HALF]] + [rcv[s, HALF] for s in range(GROUPS - 1)]
    top = functools.reduce(jnp.maximum, tiles)
    ws = [weights_of(t, top) for t in tiles]
    total = functools.reduce(jnp.add, [t * pltpu.roll(w, LANE_L, 1) for t, w in zip(tiles, ws)])
    heads = []
    for i in range(HALF):
        acc = cmb[GROUPS - 1, i] * ws[0][:, i:i + 1]
        for s in range(GROUPS - 1):
            acc += rcv[s, i] * ws[s + 1][:, i:i + 1]
        heads.append((acc / total[:, LANE_L + i:LANE_L + i + 1]).astype(BF16))
    ctx = jnp.concatenate(heads, axis=1)

    def project(column_half):
        cols = pl.ds(pl.multiple_of(HALF * HD * column_half, HD), HALF * HD)
        return (jnp.dot(ctx[:, :FF], wu[:, cols], preferred_element_type=F32)
                + jnp.dot(ctx[:, FF:], wd[:, cols], preferred_element_type=F32))

    c_o[0].wait()
    c_o[1].wait()
    other = project(1 - core)
    for i in range(HALF):
        wsend[i] = other[:, HD * i:HD * (i + 1)]
    r_wo = remote(wsend, wrecv, wo_s, wo_r, partner)
    r_wo.start()
    mine = project(core)
    r_wo.wait_recv()
    for i in range(HALF):
        agb[chip, core, i] = mine[:, HD * i:HD * (i + 1)] + wrecv[i] + fin[i]

    def piece(zz, yy):
        return agb.at[zz * 2 + yy, core]

    def send_z(d):
        return remote(piece(z, y), piece(z, y), agz_s.at[d - 1], agz_r.at[d - 1], zpeer(d))

    def send_y(d):
        zz = (z + 4 - d) % 4
        return remote(piece(zz, y), piece(zz, y), agy_s.at[d], agy_r.at[d], ypeer)

    def send_c(d, other_y):
        zz = (z + 4 - d) % 4
        yy = (y + other_y) % 2
        return remote(piece(zz, yy), piece(zz, yy), agc_s.at[2 * d + other_y], agc_r.at[2 * d + other_y], partner)

    for d in (2, 1, 3):
        send_z(d).start()
    send_y(0).start()
    send_c(0, 0).start()
    for d in (1, 2, 3):
        send_z(d).wait_recv()
        send_y(d).start()
        send_c(d, 0).start()
    for d in range(4):
        send_y(d).wait_recv()
        send_c(d, 1).start()
    for d in range(4):
        for o in range(2):
            send_c(d, o).wait_recv()

    r_mld.wait_send()
    r_mly.wait_send()
    for c in r_mlz:
        c.wait_send()
    for s in range(GROUPS):
        r_d2d(s).wait_send()
    for s in range(GROUPS - 1):
        r_a2a(s).wait_send()
    r_wo.wait_send()
    for d in (1, 2, 3):
        send_z(d).wait_send()
    for d in range(4):
        send_y(d).wait_send()
        send_c(d, 0).wait_send()
        send_c(d, 1).wait_send()


def write_kernel(pos, ko, vo, kn, vn, agb, x_ref, out_ref, k_out, v_out, kw, vw, sem):
    me = lax.axis_index("sp")
    sub = lax.broadcasted_iota(jnp.int32, (16, HD), 0)
    copies = []
    for i in range(GROUPS):
        for r in range(8):
            b = 8 * i + r
            local = pos[b] - me * SEQ

            @pl.when((local >= 0) & (local < SEQ))
            def _():
                tile = pl.ds(pl.multiple_of(local // 16 * 16, 16), 16)
                here = sub == local % 16
                kw[b, tile, :] = jnp.where(here, kn[i, r:r + 1, :], ko[b, tile, :].astype(F32)).astype(BF16)
                vw[b, tile, :] = jnp.where(here, vn[i, r:r + 1, :], vo[b, tile, :].astype(F32)).astype(BF16)

        rows = pl.ds(8 * i, 8)
        copies.append(pltpu.make_async_copy(kw.at[rows], k_out.at[rows], sem.at[2 * i]))
        copies.append(pltpu.make_async_copy(vw.at[rows], v_out.at[rows], sem.at[2 * i + 1]))
        copies[-2].start()
        copies[-1].start()
    for q in range(GROUPS // 2):
        rows = slice(16 * q, 16 * (q + 1))
        for j in range(NH):
            cols = slice(HD * j, HD * (j + 1))
            both = agb[2 * q:2 * q + 2, j // HALF, j % HALF].reshape(16, HD)
            out_ref[rows, cols] = (x_ref[rows, cols].astype(F32) + both).astype(BF16)
    for c in copies:
        c.wait()


def in_hbm(array):
    return pltpu.with_memory_space_constraint(array, pltpu.HBM)


def in_vmem(array):
    return pltpu.with_memory_space_constraint(array, pltpu.VMEM)


def device_step(hidden, ln_gamma, ln_beta, w_qkv, w_out, w_up, w_down, k_cache, v_cache, positions):
    pair_ids = np.arange(0, HD, 2, dtype=np.float64) / HD
    freq = jnp.asarray(np.tile(ROPE_BASE ** -pair_ids, 2)[None], F32)

    vmem = pl.BlockSpec(memory_space=pltpu.VMEM)
    hbm = pl.BlockSpec(memory_space=pltpu.HBM)
    dma = pltpu.SemaphoreType.DMA
    agb, k_blk, v_blk, k_row, v_row = pl.pallas_call(
        main_kernel,
        out_shape=(
            pltpu.VMEM((GROUPS, 2, HALF, 8, HD), F32),
            pltpu.VMEM(k_cache.shape, BF16),
            pltpu.VMEM(v_cache.shape, BF16),
            pltpu.VMEM((GROUPS, 8, HD), F32),
            pltpu.VMEM((GROUPS, 8, HD), F32),
        ),
        in_specs=[hbm] * 11,
        out_specs=(vmem,) * 5,
        scratch_shapes=[
            pltpu.SMEM((ROWS,), jnp.int32),
            pltpu.VMEM((ROWS, D), BF16),
            pltpu.VMEM((D,), F32),
            pltpu.VMEM((D,), F32),
            pltpu.VMEM((1, HD), F32),
            pltpu.VMEM((ROWS, HD), jnp.int32),
            pltpu.VMEM((QSLOTS, D, QCHUNK), BF16),
            pltpu.VMEM((FF, D), BF16),
            pltpu.VMEM((FF, D), BF16),
            pltpu.VMEM((ROWS, D), BF16),
            pltpu.VMEM((ROWS, FF), BF16),
            pltpu.VMEM((GROUPS, NH, 8, HD), F32),
            pltpu.VMEM((GROUPS, 2, HALF + 1, 8, HD), F32),
            pltpu.VMEM((GROUPS, HALF + 1, 8, HD), F32),
            pltpu.VMEM((GROUPS, HALF + 1, 8, HD), F32),
            pltpu.VMEM((GROUPS - 1, HALF + 1, 8, HD), F32),
            pltpu.VMEM((GROUPS, 2, HALF, 8, HD), F32),
            pltpu.VMEM((GROUPS, HALF, 8, HD), F32),
            pltpu.VMEM((4, 2, HALF, 8, HD), F32),
            pltpu.VMEM((4, HALF, 8, HD), F32),
            pltpu.VMEM((4, HALF, 8, HD), F32),
            pltpu.VMEM((3, HALF, 8, HD), F32),
            pltpu.VMEM((HALF, 8, HD), F32),
            pltpu.VMEM((HALF, 8, HD), F32),
            dma((5,)), dma((2,)), dma((NQ,)), dma((2,)), dma((GROUPS,)), dma((GROUPS,)),
            dma((GROUPS,)), dma((GROUPS,)), dma((GROUPS - 1,)), dma((GROUPS - 1,)),
            dma, dma, dma, dma, dma((3,)), dma((3,)), dma, dma,
            dma((3,)), dma((3,)), dma((4,)), dma((4,)), dma((8,)), dma((8,)),
        ],
        compiler_params=pltpu.CompilerParams(collective_id=0, has_side_effects=True, vmem_limit_bytes=32 * 2**20),
        name="layer",
    )(*[in_hbm(a) for a in (positions, hidden, ln_gamma, ln_beta, freq,
                               w_qkv, w_out, w_up.T, w_down, k_cache, v_cache)])

    out, k_new, v_new, _, _ = pl.pallas_call(
        write_kernel,
        out_shape=(
            jax.ShapeDtypeStruct(hidden.shape, BF16),
            jax.ShapeDtypeStruct(k_cache.shape, BF16),
            jax.ShapeDtypeStruct(v_cache.shape, BF16),
            pltpu.VMEM(k_cache.shape, BF16),
            pltpu.VMEM(v_cache.shape, BF16),
        ),
        in_specs=[pl.BlockSpec(memory_space=pltpu.SMEM)] + [vmem] * 6,
        out_specs=(vmem, hbm, hbm, vmem, vmem),
        scratch_shapes=[dma((2 * GROUPS,))],
        input_output_aliases={1: 3, 2: 4},
        compiler_params=pltpu.CompilerParams(vmem_limit_bytes=16 * 2**20),
        name="write",
    )(positions, *[in_vmem(a) for a in (k_blk, v_blk, k_row, v_row, agb)], hidden)
    return out, k_new, v_new


def solution(mesh):
    cache_spec = P('dp', 'sp', None)
    in_specs = (P('dp', None), P(None), P(None), P(None, None), P(None, None), P(None, 'sp'), P('sp', None), cache_spec, cache_spec, P('dp'))
    out_specs = (P('dp', None), cache_spec, cache_spec)
    return jax.shard_map(device_step, mesh=mesh, in_specs=in_specs, out_specs=out_specs, check_vma=False)
```

```python
import functools
import math

import jax
import jax.numpy as jnp
import numpy as np
from jax import lax
from jax.experimental import pallas as pl
from jax.experimental.pallas import tpu as pltpu
from jax.sharding import PartitionSpec as P

LN_EPS = 1e-5
ROPE_BASE = 10000.0
NEG_FILL = -1e30
MESH = pl.DeviceIdType.MESH

ROWS = 64
D = 2816
HD = 128
NH = 22
HALF = 11
FF = 704
SEQ = 512
GROUPS = 8
LANE_L = 64
QCHUNK = 512
NQ = 6
QSLOTS = 4
F32 = jnp.float32
BF16 = jnp.bfloat16


def rope(vec, cos, sin_signed):
    return (vec * cos + pltpu.roll(vec, HD // 2, 1) * sin_signed).astype(BF16).astype(F32)


def remote(src, dst, ssem, rsem, dev):
    return pltpu.make_async_remote_copy(src, dst, ssem, rsem, device_id=dev, device_id_type=MESH)


def weights_of(tile, top):
    return jnp.exp(tile - top)


def main_kernel(pos_h, x_h, g_h, b_h, freq_h, wqkv, wout, wup, wdn, kh, vh,
                agb, ko, vo, kn, vn,
                pos, x_s, g_s, b_s, freq_s, posv, wq, wu, wd, h_s, act, q4,
                st, d2d, cmb, yrcv, zsnd, zrcv, ml, mld, mls, mly, mlz, mlr, wsend, wrecv,
                isem, wsem, qsem, osem, ksem, vsem,
                d2d_s, d2d_r, sty_s, sty_r, stz_s, stz_r, mld_s, mld_r, mly_s, mly_r, mlz_s, mlz_r, wo_s, wo_r,
                agz_s, agz_r, agy_s, agy_r, agc_s, agc_r):
    dp = lax.axis_index("dp")
    me = lax.axis_index("sp")
    core = me % 2
    chip = me // 2
    y = chip % 2
    z = chip // 2
    partner = (dp, me + 1 - 2 * core)
    ypeer = (dp, me + 2 - 4 * y)

    def zpeer(d):
        return (dp, ((z + d) % 4) * 4 + y * 2 + core)

    c_in = [pltpu.make_async_copy(src, dst, isem.at[i])
            for i, (src, dst) in enumerate(((x_h, x_s), (g_h, g_s), (b_h, b_s), (freq_h, freq_s), (pos_h, pos)))]
    c_up = pltpu.make_async_copy(wup, wu, wsem.at[0])
    c_dn = pltpu.make_async_copy(wdn, wd, wsem.at[1])
    c_q = [pltpu.make_async_copy(wqkv.at[:, pl.ds(QCHUNK * i, QCHUNK)], wq.at[i % QSLOTS], qsem.at[i]) for i in range(NQ)]

    def group(s):
        return ((z + s // 2 + 1) % 4) * 2 + (y + s + 1) % 2

    def c_kv(s):
        rows = pl.ds(8 * group(s), 8)
        return (pltpu.make_async_copy(kh.at[rows], ko.at[rows], ksem.at[s]),
                pltpu.make_async_copy(vh.at[rows], vo.at[rows], vsem.at[s]))

    def start_kv(s):
        for c in c_kv(s):
            c.start()

    c_o = [pltpu.make_async_copy(wout.at[pl.ds((2 * core + i) * FF, FF)], (wu, wd)[i], osem.at[i]) for i in range(2)]

    for c in c_in + [c_up, c_dn]:
        c.start()
    for i in range(3):
        c_q[i].start()

    barrier = pltpu.get_barrier_semaphore()
    pl.semaphore_signal(barrier, inc=1, device_id=partner, device_id_type=MESH)
    pl.semaphore_signal(barrier, inc=1, device_id=ypeer, device_id_type=MESH)
    for d in range(1, 4):
        pl.semaphore_signal(barrier, inc=1, device_id=zpeer(d), device_id_type=MESH)

    for c in c_in:
        c.wait()
    gamma = g_s[...].reshape(1, D)
    beta = b_s[...].reshape(1, D)

    def norm_rows(i, carry):
        rows = pl.ds(pl.multiple_of(16 * i, 16), 16)
        xf = x_s[rows, :].astype(F32)
        cen = xf - jnp.mean(xf, axis=-1, keepdims=True)
        var = jnp.mean(cen * cen, axis=-1, keepdims=True)
        h_s[rows, :] = (cen * lax.rsqrt(var + LN_EPS) * gamma + beta).astype(BF16)
        return carry

    lax.fori_loop(0, ROWS // 16, norm_rows, 0)

    for b in range(ROWS):
        posv[b:b + 1, :] = jnp.full((1, HD), pos[b], jnp.int32)
    angles = posv[...].astype(F32) * freq_s[...]
    cos = jnp.cos(angles)
    sin = jnp.sin(angles)
    sin = jnp.where(lax.broadcasted_iota(jnp.int32, (ROWS, HD), 1) < HD // 2, -sin, sin)

    c_up.wait()
    c_q[3].start()
    up = lax.dot_general(h_s[...], wu[...], (((1,), (1,)), ((), ())), preferred_element_type=F32)
    act[...] = (0.5 * up * (1.0 + lax.erf(up * (1.0 / math.sqrt(2.0))))).astype(BF16)
    c_dn.wait()
    for n in range(HALF):
        part = jnp.dot(act[...], wd[:, 256 * n:256 * (n + 1)], preferred_element_type=F32)
        for j in (2 * n, 2 * n + 1):
            ml[:, j // HALF, j % HALF] = part[:, 128 * (j - 2 * n):128 * (j - 2 * n + 1)].reshape(GROUPS, 8, HD)
    pl.semaphore_wait(barrier, 5)
    r_mld = remote(ml.at[:, 1 - core], mld, mld_s, mld_r, partner)
    r_mld.start()


    def r_mly(j):
        zt = (z + j + 1) % 4
        return remote(mls.at[zt, 1 - y], mly.at[j], mly_s.at[j], mly_r.at[j], ypeer)

    def r_mlz(j):
        return remote(mlz.at[j], mlr.at[j], mlz_s.at[j], mlz_r.at[j], zpeer(j + 1))

    def mlp_z(j):
        r_mly(j).wait_recv()
        mlz[j] = mls[(z + j + 1) % 4, y] + mly[j]

    for ch in range(NQ):
        c_q[ch].wait()
        acc = jnp.dot(h_s[...], wq[ch % QSLOTS], preferred_element_type=F32).astype(BF16).astype(F32)
        if ch + QSLOTS < NQ:
            c_q[ch + QSLOTS].start()
        if ch >= 2:
            start_kv(ch - 2)
        for i in range(QCHUNK // HD):
            h = ch * (QCHUNK // HD) + i
            vec = acc[:, HD * i:HD * (i + 1)]
            if h <= NH:
                vec = rope(vec, cos, sin)
            vec = vec.reshape(GROUPS, 8, HD)
            if h < NH:
                q4[:, h] = vec
            elif h == NH:
                kn[...] = vec
            else:
                vn[...] = vec
        if ch == 1:
            r_mld.wait_recv()
            mls[...] = ml[:, core].reshape(4, 2, HALF, 8, HD) + mld[...].reshape(4, 2, HALF, 8, HD)
            for j in range(4):
                r_mly(j).start()

    col_id = lax.broadcasted_iota(jnp.int32, (NH, SEQ), 1)
    sub = lax.broadcasted_iota(jnp.int32, (NH, HD), 0)
    lane = lax.broadcasted_iota(jnp.int32, (NH, HD), 1)

    def attend(s):
        p = group(s)
        local = [pos[8 * p + r] - me * SEQ for r in range(8)]
        inside = [(x >= 0) & (x < SEQ) for x in local]
        qs = [q4[p, :, r, :] for r in range(8)]
        scores = [lax.dot_general(qs[r].astype(BF16), ko[8 * p + r], (((1,), (1,)), ((), ())), preferred_element_type=F32)
                  for r in range(8)]
        s_new = [jnp.sum(qs[r] * kn[p, r:r + 1, :], axis=-1, keepdims=True) * HD ** -0.5 for r in range(8)]
        s_new = [jnp.where(inside[r], s_new[r], NEG_FILL) for r in range(8)]
        masked = [jnp.where(col_id < local[r], scores[r] * HD ** -0.5, NEG_FILL) for r in range(8)]
        ms = [jnp.maximum(jnp.max(masked[r], axis=-1, keepdims=True), s_new[r]) for r in range(8)]
        es = [jnp.where(col_id < local[r], jnp.exp(masked[r] - ms[r]), 0.0) for r in range(8)]
        e_new = [jnp.where(inside[r], jnp.exp(s_new[r] - ms[r]), 0.0) for r in range(8)]
        os = [jnp.dot(es[r].astype(BF16), vo[8 * p + r], preferred_element_type=F32) for r in range(8)]
        ls = [jnp.sum(es[r], axis=-1, keepdims=True) + e_new[r] for r in range(8)]
        for r in range(8):
            o = os[r] + e_new[r].astype(BF16).astype(F32) * vn[p, r:r + 1, :]
            for half in range(2):
                idx = sub - HALF * half
                own = (idx >= 0) & (idx < HALF)
                t = jnp.where(own & (lane == idx), ms[r], jnp.where(own & (lane == idx + LANE_L), ls[r], 0.0))
                st[s, half, HALF, r:r + 1, :] = jnp.sum(t, axis=0, keepdims=True)
                st[s, half, 0:HALF, r, :] = o[HALF * half:HALF * (half + 1), :]

    def r_d2d(s):
        return remote(st.at[s, 1 - core], d2d.at[s], d2d_s.at[s], d2d_r.at[s], partner)

    def r_y(j):
        return remote(cmb.at[2 * j], yrcv.at[j], sty_s.at[j], sty_r.at[j], ypeer)

    def r_z(j):
        return remote(zsnd.at[j], zrcv.at[j], stz_s.at[j], stz_r.at[j], zpeer(j + 1))

    lane8 = lax.broadcasted_iota(jnp.int32, (8, HD), 1)

    def merge(dst, a, b):
        ta, tb = a[HALF], b[HALF]
        top = jnp.maximum(ta, tb)
        wa, wb = weights_of(ta, top), weights_of(tb, top)
        total = ta * pltpu.roll(wa, LANE_L, 1) + tb * pltpu.roll(wb, LANE_L, 1)
        dst[HALF] = jnp.where(lane8 < LANE_L, top, total)
        for i in range(HALF):
            dst[i] = a[i] * wa[:, i:i + 1] + b[i] * wb[:, i:i + 1]

    def pair(s):
        r_d2d(s).wait_recv()
        merge(cmb.at[s], st.at[s, core], d2d.at[s])

    def pair_y(j):
        r_y(j).wait_recv()
        merge(zsnd.at[j], cmb.at[2 * j + 1], yrcv.at[j])

    def step(s, carry):
        ck, cv = c_kv(s)
        ck.wait()
        cv.wait()

        @pl.when(s < 4)
        def _():
            start_kv(s + 4)

        @pl.when(s == 4)
        def _():
            c_o[0].start()

        @pl.when(s == 5)
        def _():
            c_o[1].start()

        attend(s)
        r_d2d(s).start()

        @pl.when(s > 0)
        def _():
            pair(s - 1)

        @pl.when(s % 2 == 1)
        def _():
            r_y(s // 2).start()

        @pl.when((s >= 2) & (s < 5))
        def _():
            mlp_z(s - 2)
            r_mlz(s - 2).start()

        @pl.when((s == 5) | (s == 7))
        def _():
            pair_y((s - 5) // 2)
            r_z((s - 5) // 2).start()

        return carry

    lax.fori_loop(0, GROUPS, step, 0)
    pair(GROUPS - 1)
    pair_y(2)
    r_z(2).start()

    mlp_z(3)
    pair_y(3)
    for j in range(3):
        r_z(j).wait_recv()
    parts = [zsnd.at[3], zrcv.at[0], zrcv.at[1], zrcv.at[2]]
    tiles = [part[HALF] for part in parts]
    top = functools.reduce(jnp.maximum, tiles)
    ws = [weights_of(t, top) for t in tiles]
    total = functools.reduce(jnp.add, [t * pltpu.roll(w, LANE_L, 1) for t, w in zip(tiles, ws)])
    heads = []
    for i in range(HALF):
        acc = functools.reduce(jnp.add, [part[i] * w[:, i:i + 1] for part, w in zip(parts, ws)])
        heads.append((acc / total[:, LANE_L + i:LANE_L + i + 1]).astype(BF16))
    ctx = jnp.concatenate(heads, axis=1)

    def project(column_half):
        cols = pl.ds(pl.multiple_of(HALF * HD * column_half, HD), HALF * HD)
        return (jnp.dot(ctx[:, :FF], wu[:, cols], preferred_element_type=F32)
                + jnp.dot(ctx[:, FF:], wd[:, cols], preferred_element_type=F32))

    c_o[0].wait()
    c_o[1].wait()
    other = project(1 - core)
    for i in range(HALF):
        wsend[i] = other[:, HD * i:HD * (i + 1)]
    r_wo = remote(wsend, wrecv, wo_s, wo_r, partner)
    r_wo.start()
    mine = project(core)
    for j in range(3):
        r_mlz(j).wait_recv()
    fin = mlz[3] + mlr[0] + mlr[1] + mlr[2]
    r_wo.wait_recv()
    for i in range(HALF):
        agb[chip, core, i] = mine[:, HD * i:HD * (i + 1)] + wrecv[i] + fin[i]

    def piece(zz, yy):
        return agb.at[zz * 2 + yy, core]

    def send_z(d):
        return remote(piece(z, y), piece(z, y), agz_s.at[d - 1], agz_r.at[d - 1], zpeer(d))

    def send_y(d):
        zz = (z + 4 - d) % 4
        return remote(piece(zz, y), piece(zz, y), agy_s.at[d], agy_r.at[d], ypeer)

    def send_c(d, other_y):
        zz = (z + 4 - d) % 4
        yy = (y + other_y) % 2
        return remote(piece(zz, yy), piece(zz, yy), agc_s.at[2 * d + other_y], agc_r.at[2 * d + other_y], partner)

    flip = z // 2
    near = z + flip * (3 - 2 * z)
    order = [src + flip * (3 - 2 * src) for src in (1 - near, 2, 3)]
    dist = [(z + 4 - src) % 4 for src in order]
    for i in (2, 1, 0):
        send_z((order[i] + 4 - z) % 4).start()
    send_y(0).start()
    send_c(0, 0).start()
    for i in range(3):
        send_z(dist[i]).wait_recv()
        send_y(dist[i]).start()
        send_c(dist[i], 0).start()
        back = 0 if i == 0 else dist[i - 1]
        send_y(back).wait_recv()
        send_c(back, 1).start()
    send_y(dist[2]).wait_recv()
    send_c(dist[2], 1).start()
    for d in range(4):
        for o in range(2):
            send_c(d, o).wait_recv()

    r_mld.wait_send()
    for s in range(GROUPS):
        r_d2d(s).wait_send()
    for j in range(4):
        r_mly(j).wait_send()
        r_y(j).wait_send()
    for j in range(3):
        r_mlz(j).wait_send()
        r_z(j).wait_send()
    r_wo.wait_send()
    for d in (1, 2, 3):
        send_z(d).wait_send()
    for d in range(4):
        send_y(d).wait_send()
        send_c(d, 0).wait_send()
        send_c(d, 1).wait_send()


def write_kernel(pos, ko, vo, kn, vn, agb, x_ref, out_ref, k_out, v_out, kw, vw, sem):
    me = lax.axis_index("sp")
    sub = lax.broadcasted_iota(jnp.int32, (16, HD), 0)
    copies = []
    for i in range(GROUPS):
        for r in range(8):
            b = 8 * i + r
            local = pos[b] - me * SEQ

            @pl.when((local >= 0) & (local < SEQ))
            def _():
                tile = pl.ds(pl.multiple_of(local // 16 * 16, 16), 16)
                here = sub == local % 16
                kw[b, tile, :] = jnp.where(here, kn[i, r:r + 1, :], ko[b, tile, :].astype(F32)).astype(BF16)
                vw[b, tile, :] = jnp.where(here, vn[i, r:r + 1, :], vo[b, tile, :].astype(F32)).astype(BF16)

        rows = pl.ds(8 * i, 8)
        copies.append(pltpu.make_async_copy(kw.at[rows], k_out.at[rows], sem.at[2 * i]))
        copies.append(pltpu.make_async_copy(vw.at[rows], v_out.at[rows], sem.at[2 * i + 1]))
        copies[-2].start()
        copies[-1].start()
    for q in range(GROUPS // 2):
        rows = slice(16 * q, 16 * (q + 1))
        for j in range(NH):
            cols = slice(HD * j, HD * (j + 1))
            both = agb[2 * q:2 * q + 2, j // HALF, j % HALF].reshape(16, HD)
            out_ref[rows, cols] = (x_ref[rows, cols].astype(F32) + both).astype(BF16)
    for c in copies:
        c.wait()


def in_hbm(array):
    return pltpu.with_memory_space_constraint(array, pltpu.HBM)


def in_vmem(array):
    return pltpu.with_memory_space_constraint(array, pltpu.VMEM)


def device_step(hidden, ln_gamma, ln_beta, w_qkv, w_out, w_up, w_down, k_cache, v_cache, positions):
    pair_ids = np.arange(0, HD, 2, dtype=np.float64) / HD
    freq = jnp.asarray(np.tile(ROPE_BASE ** -pair_ids, 2)[None], F32)

    vmem = pl.BlockSpec(memory_space=pltpu.VMEM)
    hbm = pl.BlockSpec(memory_space=pltpu.HBM)
    dma = pltpu.SemaphoreType.DMA
    agb, k_blk, v_blk, k_row, v_row = pl.pallas_call(
        main_kernel,
        out_shape=(
            pltpu.VMEM((GROUPS, 2, HALF, 8, HD), F32),
            pltpu.VMEM(k_cache.shape, BF16),
            pltpu.VMEM(v_cache.shape, BF16),
            pltpu.VMEM((GROUPS, 8, HD), F32),
            pltpu.VMEM((GROUPS, 8, HD), F32),
        ),
        in_specs=[hbm] * 11,
        out_specs=(vmem,) * 5,
        scratch_shapes=[
            pltpu.SMEM((ROWS,), jnp.int32),
            pltpu.VMEM((ROWS, D), BF16),
            pltpu.VMEM((D,), F32),
            pltpu.VMEM((D,), F32),
            pltpu.VMEM((1, HD), F32),
            pltpu.VMEM((ROWS, HD), jnp.int32),
            pltpu.VMEM((QSLOTS, D, QCHUNK), BF16),
            pltpu.VMEM((FF, D), BF16),
            pltpu.VMEM((FF, D), BF16),
            pltpu.VMEM((ROWS, D), BF16),
            pltpu.VMEM((ROWS, FF), BF16),
            pltpu.VMEM((GROUPS, NH, 8, HD), F32),
            pltpu.VMEM((GROUPS, 2, HALF + 1, 8, HD), F32),
            pltpu.VMEM((GROUPS, HALF + 1, 8, HD), F32),
            pltpu.VMEM((GROUPS, HALF + 1, 8, HD), F32),
            pltpu.VMEM((4, HALF + 1, 8, HD), F32),
            pltpu.VMEM((4, HALF + 1, 8, HD), F32),
            pltpu.VMEM((3, HALF + 1, 8, HD), F32),
            pltpu.VMEM((GROUPS, 2, HALF, 8, HD), F32),
            pltpu.VMEM((GROUPS, HALF, 8, HD), F32),
            pltpu.VMEM((4, 2, HALF, 8, HD), F32),
            pltpu.VMEM((4, HALF, 8, HD), F32),
            pltpu.VMEM((4, HALF, 8, HD), F32),
            pltpu.VMEM((3, HALF, 8, HD), F32),
            pltpu.VMEM((HALF, 8, HD), F32),
            pltpu.VMEM((HALF, 8, HD), F32),
            dma((5,)), dma((2,)), dma((NQ,)), dma((2,)), dma((GROUPS,)), dma((GROUPS,)),
            dma((GROUPS,)), dma((GROUPS,)), dma((4,)), dma((4,)), dma((3,)), dma((3,)),
            dma, dma, dma((4,)), dma((4,)), dma((3,)), dma((3,)), dma, dma,
            dma((3,)), dma((3,)), dma((4,)), dma((4,)), dma((8,)), dma((8,)),
        ],
        compiler_params=pltpu.CompilerParams(collective_id=0, has_side_effects=True, vmem_limit_bytes=32 * 2**20),
        name="layer",
    )(*[in_hbm(a) for a in (positions, hidden, ln_gamma, ln_beta, freq,
                               w_qkv, w_out, w_up.T, w_down, k_cache, v_cache)])

    out, k_new, v_new, _, _ = pl.pallas_call(
        write_kernel,
        out_shape=(
            jax.ShapeDtypeStruct(hidden.shape, BF16),
            jax.ShapeDtypeStruct(k_cache.shape, BF16),
            jax.ShapeDtypeStruct(v_cache.shape, BF16),
            pltpu.VMEM(k_cache.shape, BF16),
            pltpu.VMEM(v_cache.shape, BF16),
        ),
        in_specs=[pl.BlockSpec(memory_space=pltpu.SMEM)] + [vmem] * 6,
        out_specs=(vmem, hbm, hbm, vmem, vmem),
        scratch_shapes=[dma((2 * GROUPS,))],
        input_output_aliases={1: 3, 2: 4},
        compiler_params=pltpu.CompilerParams(vmem_limit_bytes=16 * 2**20),
        name="write",
    )(positions, *[in_vmem(a) for a in (k_blk, v_blk, k_row, v_row, agb)], hidden)
    return out, k_new, v_new


def solution(mesh):
    cache_spec = P('dp', 'sp', None)
    in_specs = (P('dp', None), P(None), P(None), P(None, None), P(None, None), P(None, 'sp'), P('sp', None), cache_spec, cache_spec, P('dp'))
    out_specs = (P('dp', None), cache_spec, cache_spec)
    return jax.shard_map(device_step, mesh=mesh, in_specs=in_specs, out_specs=out_specs, check_vma=False)
```

```python
import functools
import math

import jax
import jax.numpy as jnp
import numpy as np
from jax import lax
from jax.experimental import pallas as pl
from jax.experimental.pallas import tpu as pltpu
from jax.sharding import PartitionSpec as P

LN_EPS = 1e-5
ROPE_BASE = 10000.0
NEG_FILL = -1e30
MESH = pl.DeviceIdType.MESH

ROWS = 64
D = 2816
HD = 128
NH = 22
HALF = 11
FF = 704
SEQ = 512
GROUPS = 8
LANE_L = 64
QCHUNK = 512
NQ = 6
QSLOTS = 4
F32 = jnp.float32
BF16 = jnp.bfloat16


def rope(vec, cos, sin_signed):
    return (vec * cos + pltpu.roll(vec, HD // 2, 1) * sin_signed).astype(BF16).astype(F32)


def remote(src, dst, ssem, rsem, dev):
    return pltpu.make_async_remote_copy(src, dst, ssem, rsem, device_id=dev, device_id_type=MESH)


def weights_of(tile, top):
    return jnp.exp(tile - top)


def main_kernel(pos_h, x_h, g_h, b_h, freq_h, wqkv, wout, wup, wdn, kh, vh,
                agb, ko, vo, kn, vn,
                pos, x_s, g_s, b_s, freq_s, posv, wq, wu, wd, h_s, act, q4,
                st, d2d, cmb, yrcv, zsnd, zrcv, ml, mld, mls, mly, mlz, mlr, wsend, wrecv,
                isem, wsem, qsem, osem, ksem, vsem,
                d2d_s, d2d_r, sty_s, sty_r, stz_s, stz_r, mld_s, mld_r, mly_s, mly_r, mlz_s, mlz_r, wo_s, wo_r,
                agz_s, agz_r, agy_s, agy_r, agc_s, agc_r):
    dp = lax.axis_index("dp")
    me = lax.axis_index("sp")
    core = me % 2
    chip = me // 2
    y = chip % 2
    z = chip // 2
    partner = (dp, me + 1 - 2 * core)
    ypeer = (dp, me + 2 - 4 * y)

    def zpeer(d):
        return (dp, ((z + d) % 4) * 4 + y * 2 + core)

    c_in = [pltpu.make_async_copy(src, dst, isem.at[i])
            for i, (src, dst) in enumerate(((x_h, x_s), (g_h, g_s), (b_h, b_s), (freq_h, freq_s), (pos_h, pos)))]
    c_up = pltpu.make_async_copy(wup, wu, wsem.at[0])
    c_dn = pltpu.make_async_copy(wdn, wd, wsem.at[1])
    c_q = [pltpu.make_async_copy(wqkv.at[:, pl.ds(QCHUNK * i, QCHUNK)], wq.at[i % QSLOTS], qsem.at[i]) for i in range(NQ)]

    def group(s):
        return ((z + s + 1) % 4) * 2 + (y + s // 4 + 1) % 2

    def c_kv(s):
        rows = pl.ds(8 * group(s), 8)
        return (pltpu.make_async_copy(kh.at[rows], ko.at[rows], ksem.at[s]),
                pltpu.make_async_copy(vh.at[rows], vo.at[rows], vsem.at[s]))

    def start_kv(s):
        for c in c_kv(s):
            c.start()

    c_o = [pltpu.make_async_copy(wout.at[pl.ds((2 * core + i) * FF, FF)], (wu, wd)[i], osem.at[i]) for i in range(2)]

    for c in c_in + [c_up, c_dn]:
        c.start()
    for i in range(3):
        c_q[i].start()

    barrier = pltpu.get_barrier_semaphore()
    pl.semaphore_signal(barrier, inc=1, device_id=partner, device_id_type=MESH)
    pl.semaphore_signal(barrier, inc=1, device_id=ypeer, device_id_type=MESH)
    for d in range(1, 4):
        pl.semaphore_signal(barrier, inc=1, device_id=zpeer(d), device_id_type=MESH)

    for c in c_in[:3]:
        c.wait()
    gamma = g_s[...].reshape(1, D)
    beta = b_s[...].reshape(1, D)

    def norm_rows(i, carry):
        rows = pl.ds(pl.multiple_of(16 * i, 16), 16)
        xf = x_s[rows, :].astype(F32)
        cen = xf - jnp.mean(xf, axis=-1, keepdims=True)
        var = jnp.mean(cen * cen, axis=-1, keepdims=True)
        h_s[rows, :] = (cen * lax.rsqrt(var + LN_EPS) * gamma + beta).astype(BF16)
        return carry

    lax.fori_loop(0, ROWS // 16, norm_rows, 0)

    for c in c_in[3:]:
        c.wait()
    for b in range(ROWS):
        posv[b:b + 1, :] = jnp.full((1, HD), pos[b], jnp.int32)
    angles = posv[...].astype(F32) * freq_s[...]
    cos = jnp.cos(angles)
    sin = jnp.sin(angles)
    sin = jnp.where(lax.broadcasted_iota(jnp.int32, (ROWS, HD), 1) < HD // 2, -sin, sin)

    c_up.wait()
    c_q[3].start()
    up = lax.dot_general(h_s[...], wu[...], (((1,), (1,)), ((), ())), preferred_element_type=F32)
    act[...] = (0.5 * up * (1.0 + lax.erf(up * (1.0 / math.sqrt(2.0))))).astype(BF16)
    c_dn.wait()

    def down(column_half, dst):
        cols = pl.ds(pl.multiple_of(HALF * HD * column_half, HD), HALF * HD)
        part = jnp.dot(act[...], wd[:, cols], preferred_element_type=F32)
        for j in range(HALF):
            dst[:, j] = part[:, HD * j:HD * (j + 1)].reshape(GROUPS, 8, HD)

    down(1 - core, ml.at[0])
    pl.semaphore_wait(barrier, 5)
    r_mld = remote(ml.at[0], mld, mld_s, mld_r, partner)
    r_mld.start()
    down(core, ml.at[1])


    def r_mly(j):
        zt = (z + j + 1) % 4
        return remote(mls.at[zt, 1 - y], mly.at[j], mly_s.at[j], mly_r.at[j], ypeer)

    def r_mlz(j):
        return remote(mlz.at[j], mlr.at[j], mlz_s.at[j], mlz_r.at[j], zpeer(j + 1))

    def mlp_z(j):
        r_mly(j).wait_recv()
        mlz[j] = mls[(z + j + 1) % 4, y] + mly[j]

    for ch in range(NQ):
        c_q[ch].wait()
        acc = jnp.dot(h_s[...], wq[ch % QSLOTS], preferred_element_type=F32).astype(BF16).astype(F32)
        if ch + QSLOTS < NQ:
            c_q[ch + QSLOTS].start()
        if ch >= 2:
            start_kv(ch - 2)
        for i in range(QCHUNK // HD):
            h = ch * (QCHUNK // HD) + i
            vec = acc[:, HD * i:HD * (i + 1)]
            if h <= NH:
                vec = rope(vec, cos, sin)
            vec = vec.reshape(GROUPS, 8, HD)
            if h < NH:
                q4[:, h] = vec
            elif h == NH:
                kn[...] = vec
            else:
                vn[...] = vec
        if ch == 1:
            r_mld.wait_recv()
            mls[...] = ml[1].reshape(4, 2, HALF, 8, HD) + mld[...].reshape(4, 2, HALF, 8, HD)
            for j in range(4):
                r_mly(j).start()

    col_id = lax.broadcasted_iota(jnp.int32, (NH, SEQ), 1)
    sub = lax.broadcasted_iota(jnp.int32, (NH, HD), 0)
    lane = lax.broadcasted_iota(jnp.int32, (NH, HD), 1)

    def attend(s):
        p = group(s)
        local = [pos[8 * p + r] - me * SEQ for r in range(8)]
        inside = [(x >= 0) & (x < SEQ) for x in local]
        qs = [q4[p, :, r, :] for r in range(8)]
        scores = [lax.dot_general(qs[r].astype(BF16), ko[8 * p + r], (((1,), (1,)), ((), ())), preferred_element_type=F32)
                  for r in range(8)]
        s_new = [jnp.sum(qs[r] * kn[p, r:r + 1, :], axis=-1, keepdims=True) * HD ** -0.5 for r in range(8)]
        s_new = [jnp.where(inside[r], s_new[r], NEG_FILL) for r in range(8)]
        masked = [jnp.where(col_id < local[r], scores[r] * HD ** -0.5, NEG_FILL) for r in range(8)]
        ms = [jnp.maximum(jnp.max(masked[r], axis=-1, keepdims=True), s_new[r]) for r in range(8)]
        es = [jnp.where(col_id < local[r], jnp.exp(masked[r] - ms[r]), 0.0) for r in range(8)]
        e_new = [jnp.where(inside[r], jnp.exp(s_new[r] - ms[r]), 0.0) for r in range(8)]
        os = [jnp.dot(es[r].astype(BF16), vo[8 * p + r], preferred_element_type=F32) for r in range(8)]
        ls = [jnp.sum(es[r], axis=-1, keepdims=True) + e_new[r] for r in range(8)]
        for r in range(8):
            o = os[r] + e_new[r].astype(BF16).astype(F32) * vn[p, r:r + 1, :]
            for half in range(2):
                idx = sub - HALF * half
                own = (idx >= 0) & (idx < HALF)
                t = jnp.where(own & (lane == idx), ms[r], jnp.where(own & (lane == idx + LANE_L), ls[r], 0.0))
                st[s, half, HALF, r:r + 1, :] = jnp.sum(t, axis=0, keepdims=True)
                st[s, half, 0:HALF, r, :] = o[HALF * half:HALF * (half + 1), :]

    def r_d2d(s):
        return remote(st.at[s, 1 - core], d2d.at[s], d2d_s.at[s], d2d_r.at[s], partner)

    def r_y(j):
        return remote(cmb.at[j], yrcv.at[j], sty_s.at[j], sty_r.at[j], ypeer)

    def r_z(j):
        return remote(zsnd.at[j], zrcv.at[j], stz_s.at[j], stz_r.at[j], zpeer(j + 1))

    lane8 = lax.broadcasted_iota(jnp.int32, (8, HD), 1)

    def merge(dst, a, b):
        ta, tb = a[HALF], b[HALF]
        top = jnp.maximum(ta, tb)
        wa, wb = weights_of(ta, top), weights_of(tb, top)
        total = ta * pltpu.roll(wa, LANE_L, 1) + tb * pltpu.roll(wb, LANE_L, 1)
        dst[HALF] = jnp.where(lane8 < LANE_L, top, total)
        for i in range(HALF):
            dst[i] = a[i] * wa[:, i:i + 1] + b[i] * wb[:, i:i + 1]

    def pair(s):
        r_d2d(s).wait_recv()
        merge(cmb.at[s], st.at[s, core], d2d.at[s])

    def pair_y(j):
        r_y(j).wait_recv()
        merge(zsnd.at[j], cmb.at[4 + j], yrcv.at[j])

    def step(s, carry):
        ck, cv = c_kv(s)
        ck.wait()
        cv.wait()

        @pl.when(s < 4)
        def _():
            start_kv(s + 4)

        @pl.when(s == 4)
        def _():
            c_o[0].start()

        @pl.when(s == 5)
        def _():
            c_o[1].start()

        attend(s)
        r_d2d(s).start()

        @pl.when(s > 0)
        def _():
            pair(s - 1)

        @pl.when((s >= 1) & (s < 5))
        def _():
            r_y(s - 1).start()

        @pl.when((s >= 1) & (s < 4))
        def _():
            mlp_z(s - 1)
            r_mlz(s - 1).start()

        @pl.when(s >= 5)
        def _():
            pair_y(s - 5)
            r_z(s - 5).start()

        return carry

    lax.fori_loop(0, GROUPS, step, 0)
    mlp_z(3)
    pair(GROUPS - 1)
    pair_y(3)
    for j in range(3):
        r_z(j).wait_recv()
    parts = [zsnd.at[3], zrcv.at[0], zrcv.at[1], zrcv.at[2]]
    tiles = [part[HALF] for part in parts]
    top = functools.reduce(jnp.maximum, tiles)
    ws = [weights_of(t, top) for t in tiles]
    total = functools.reduce(jnp.add, [t * pltpu.roll(w, LANE_L, 1) for t, w in zip(tiles, ws)])
    heads = []
    for i in range(HALF):
        acc = functools.reduce(jnp.add, [part[i] * w[:, i:i + 1] for part, w in zip(parts, ws)])
        heads.append((acc / total[:, LANE_L + i:LANE_L + i + 1]).astype(BF16))
    ctx = jnp.concatenate(heads, axis=1)

    def project(column_half):
        cols = pl.ds(pl.multiple_of(HALF * HD * column_half, HD), HALF * HD)
        return (jnp.dot(ctx[:, :FF], wu[:, cols], preferred_element_type=F32)
                + jnp.dot(ctx[:, FF:], wd[:, cols], preferred_element_type=F32))

    c_o[0].wait()
    c_o[1].wait()
    other = project(1 - core)
    for i in range(HALF):
        wsend[i] = other[:, HD * i:HD * (i + 1)]
    r_wo = remote(wsend, wrecv, wo_s, wo_r, partner)
    r_wo.start()
    mine = project(core)
    for j in range(3):
        r_mlz(j).wait_recv()
    fin = mlz[3] + mlr[0] + mlr[1] + mlr[2]
    r_wo.wait_recv()
    for i in range(HALF):
        agb[chip, core, i] = mine[:, HD * i:HD * (i + 1)] + wrecv[i] + fin[i]

    def piece(zz, yy):
        return agb.at[zz * 2 + yy, core]

    def send_z(d):
        return remote(piece(z, y), piece(z, y), agz_s.at[d - 1], agz_r.at[d - 1], zpeer(d))

    def send_y(d):
        zz = (z + 4 - d) % 4
        return remote(piece(zz, y), piece(zz, y), agy_s.at[d], agy_r.at[d], ypeer)

    def send_c(d, other_y):
        zz = (z + 4 - d) % 4
        yy = (y + other_y) % 2
        return remote(piece(zz, yy), piece(zz, yy), agc_s.at[2 * d + other_y], agc_r.at[2 * d + other_y], partner)

    flip = z // 2
    near = z + flip * (3 - 2 * z)
    order = [src + flip * (3 - 2 * src) for src in (1 - near, 2, 3)]
    dist = [(z + 4 - src) % 4 for src in order]
    for i in (2, 1, 0):
        send_z((order[i] + 4 - z) % 4).start()
    send_y(0).start()
    send_c(0, 0).start()
    for d in dist:
        send_z(d).wait_recv()
        send_y(d).start()
        send_c(d, 0).start()
    for d in [0] + dist:
        send_y(d).wait_recv()
        send_c(d, 1).start()
    for d in range(4):
        for o in range(2):
            send_c(d, o).wait_recv()

    r_mld.wait_send()
    for s in range(GROUPS):
        r_d2d(s).wait_send()
    for j in range(4):
        r_mly(j).wait_send()
        r_y(j).wait_send()
    for j in range(3):
        r_mlz(j).wait_send()
        r_z(j).wait_send()
    r_wo.wait_send()
    for d in (1, 2, 3):
        send_z(d).wait_send()
    for d in range(4):
        send_y(d).wait_send()
        send_c(d, 0).wait_send()
        send_c(d, 1).wait_send()


def write_kernel(pos, ko, vo, kn, vn, agb, x_ref, out, k_out, v_out, kw, vw, out_ref, sem):
    me = lax.axis_index("sp")
    sub = lax.broadcasted_iota(jnp.int32, (16, HD), 0)
    copies = []
    for i in range(GROUPS):
        for r in range(8):
            b = 8 * i + r
            local = pos[b] - me * SEQ

            @pl.when((local >= 0) & (local < SEQ))
            def _():
                tile = pl.ds(pl.multiple_of(local // 16 * 16, 16), 16)
                here = sub == local % 16
                kw[b, tile, :] = jnp.where(here, kn[i, r:r + 1, :], ko[b, tile, :].astype(F32)).astype(BF16)
                vw[b, tile, :] = jnp.where(here, vn[i, r:r + 1, :], vo[b, tile, :].astype(F32)).astype(BF16)

        rows = pl.ds(8 * i, 8)
        copies.append(pltpu.make_async_copy(kw.at[rows], k_out.at[rows], sem.at[2 * i]))
        copies.append(pltpu.make_async_copy(vw.at[rows], v_out.at[rows], sem.at[2 * i + 1]))
        copies[-2].start()
        copies[-1].start()
    for q in range(GROUPS // 2):
        rows = slice(16 * q, 16 * (q + 1))
        for j in range(NH):
            cols = slice(HD * j, HD * (j + 1))
            both = agb[2 * q:2 * q + 2, j // HALF, j % HALF].reshape(16, HD)
            out_ref[rows, cols] = (x_ref[rows, cols].astype(F32) + both).astype(BF16)
    copies.append(pltpu.make_async_copy(out_ref, out, sem.at[2 * GROUPS]))
    copies[-1].start()
    for c in copies:
        c.wait()


def in_hbm(array):
    return pltpu.with_memory_space_constraint(array, pltpu.HBM)


def in_vmem(array):
    return pltpu.with_memory_space_constraint(array, pltpu.VMEM)


def device_step(hidden, ln_gamma, ln_beta, w_qkv, w_out, w_up, w_down, k_cache, v_cache, positions):
    pair_ids = np.arange(0, HD, 2, dtype=np.float64) / HD
    freq = jnp.asarray(np.tile(ROPE_BASE ** -pair_ids, 2)[None], F32)

    vmem = pl.BlockSpec(memory_space=pltpu.VMEM)
    hbm = pl.BlockSpec(memory_space=pltpu.HBM)
    dma = pltpu.SemaphoreType.DMA
    agb, k_blk, v_blk, k_row, v_row = pl.pallas_call(
        main_kernel,
        out_shape=(
            pltpu.VMEM((GROUPS, 2, HALF, 8, HD), F32),
            pltpu.VMEM(k_cache.shape, BF16),
            pltpu.VMEM(v_cache.shape, BF16),
            pltpu.VMEM((GROUPS, 8, HD), F32),
            pltpu.VMEM((GROUPS, 8, HD), F32),
        ),
        in_specs=[hbm] * 11,
        out_specs=(vmem,) * 5,
        scratch_shapes=[
            pltpu.SMEM((ROWS,), jnp.int32),
            pltpu.VMEM((ROWS, D), BF16),
            pltpu.VMEM((D,), F32),
            pltpu.VMEM((D,), F32),
            pltpu.VMEM((1, HD), F32),
            pltpu.VMEM((ROWS, HD), jnp.int32),
            pltpu.VMEM((QSLOTS, D, QCHUNK), BF16),
            pltpu.VMEM((FF, D), BF16),
            pltpu.VMEM((FF, D), BF16),
            pltpu.VMEM((ROWS, D), BF16),
            pltpu.VMEM((ROWS, FF), BF16),
            pltpu.VMEM((GROUPS, NH, 8, HD), F32),
            pltpu.VMEM((GROUPS, 2, HALF + 1, 8, HD), F32),
            pltpu.VMEM((GROUPS, HALF + 1, 8, HD), F32),
            pltpu.VMEM((GROUPS, HALF + 1, 8, HD), F32),
            pltpu.VMEM((4, HALF + 1, 8, HD), F32),
            pltpu.VMEM((4, HALF + 1, 8, HD), F32),
            pltpu.VMEM((3, HALF + 1, 8, HD), F32),
            pltpu.VMEM((2, GROUPS, HALF, 8, HD), F32),
            pltpu.VMEM((GROUPS, HALF, 8, HD), F32),
            pltpu.VMEM((4, 2, HALF, 8, HD), F32),
            pltpu.VMEM((4, HALF, 8, HD), F32),
            pltpu.VMEM((4, HALF, 8, HD), F32),
            pltpu.VMEM((3, HALF, 8, HD), F32),
            pltpu.VMEM((HALF, 8, HD), F32),
            pltpu.VMEM((HALF, 8, HD), F32),
            dma((5,)), dma((2,)), dma((NQ,)), dma((2,)), dma((GROUPS,)), dma((GROUPS,)),
            dma((GROUPS,)), dma((GROUPS,)), dma((4,)), dma((4,)), dma((3,)), dma((3,)),
            dma, dma, dma((4,)), dma((4,)), dma((3,)), dma((3,)), dma, dma,
            dma((3,)), dma((3,)), dma((4,)), dma((4,)), dma((8,)), dma((8,)),
        ],
        compiler_params=pltpu.CompilerParams(collective_id=0, has_side_effects=True, vmem_limit_bytes=32 * 2**20),
        name="layer",
    )(*[in_hbm(a) for a in (positions, hidden, ln_gamma, ln_beta, freq,
                               w_qkv, w_out, w_up.T, w_down, k_cache, v_cache)])

    out, k_new, v_new, _, _ = pl.pallas_call(
        write_kernel,
        out_shape=(
            jax.ShapeDtypeStruct(hidden.shape, BF16),
            jax.ShapeDtypeStruct(k_cache.shape, BF16),
            jax.ShapeDtypeStruct(v_cache.shape, BF16),
            pltpu.VMEM(k_cache.shape, BF16),
            pltpu.VMEM(v_cache.shape, BF16),
        ),
        in_specs=[pl.BlockSpec(memory_space=pltpu.SMEM)] + [vmem] * 6,
        out_specs=(hbm, hbm, hbm, vmem, vmem),
        scratch_shapes=[pltpu.VMEM((ROWS, D), BF16), dma((2 * GROUPS + 1,))],
        input_output_aliases={1: 3, 2: 4},
        compiler_params=pltpu.CompilerParams(vmem_limit_bytes=16 * 2**20),
        name="write",
    )(positions, *[in_vmem(a) for a in (k_blk, v_blk, k_row, v_row, agb)], hidden)
    return out, k_new, v_new


def solution(mesh):
    cache_spec = P('dp', 'sp', None)
    in_specs = (P('dp', None), P(None), P(None), P(None, None), P(None, None), P(None, 'sp'), P('sp', None), cache_spec, cache_spec, P('dp'))
    out_specs = (P('dp', None), cache_spec, cache_spec)
    return jax.shard_map(device_step, mesh=mesh, in_specs=in_specs, out_specs=out_specs, check_vma=False)
```

```python
import functools
import math

import jax
import jax.numpy as jnp
import numpy as np
from jax import lax
from jax.experimental import pallas as pl
from jax.experimental.pallas import tpu as pltpu
from jax.sharding import PartitionSpec as P

LN_EPS = 1e-5
ROPE_BASE = 10000.0
NEG_FILL = -1e30
MESH = pl.DeviceIdType.MESH

ROWS = 64
D = 2816
HD = 128
NH = 22
HALF = 11
FF = 704
SEQ = 512
GROUPS = 8
LANE_L = 64
QCHUNK = 512
NQ = 6
QSLOTS = 4
F32 = jnp.float32
BF16 = jnp.bfloat16


def rope(vec, cos, sin_signed):
    return (vec * cos + pltpu.roll(vec, HD // 2, 1) * sin_signed).astype(BF16).astype(F32)


def remote(src, dst, ssem, rsem, dev):
    return pltpu.make_async_remote_copy(src, dst, ssem, rsem, device_id=dev, device_id_type=MESH)


def weights_of(tile, top):
    return jnp.exp(tile - top)


def main_kernel(pos_h, x_h, g_h, b_h, freq_h, wqkv, wout, wup, wdn, kh, vh,
                agb, ko, vo, kn, vn,
                pos, x_s, g_s, b_s, freq_s, posv, wq, wu, wd, h_s, act, q4,
                st, d2d, cmb, yrcv, zsnd, zrcv, ml, mld, mls, mly, mlz, mlr, wsend, wrecv,
                isem, wsem, qsem, osem, ksem, vsem,
                d2d_s, d2d_r, sty_s, sty_r, stz_s, stz_r, mld_s, mld_r, mly_s, mly_r, mlz_s, mlz_r, wo_s, wo_r,
                agz_s, agz_r, agy_s, agy_r, agc_s, agc_r):
    dp = lax.axis_index("dp")
    me = lax.axis_index("sp")
    core = me % 2
    chip = me // 2
    y = chip % 2
    z = chip // 2
    partner = (dp, me + 1 - 2 * core)
    ypeer = (dp, me + 2 - 4 * y)

    def zpeer(d):
        return (dp, ((z + d) % 4) * 4 + y * 2 + core)

    sign = 1 - 2 * (z // 2)

    def target(j):
        return (z + 4 + sign * (j + 1)) % 4

    def target_dev(j):
        return (dp, target(j) * 4 + y * 2 + core)

    def slot(j):
        return 1 + sign * (1 - j)

    c_in = [pltpu.make_async_copy(src, dst, isem.at[i])
            for i, (src, dst) in enumerate(((x_h, x_s), (g_h, g_s), (b_h, b_s), (freq_h, freq_s), (pos_h, pos)))]
    c_up = pltpu.make_async_copy(wup, wu, wsem.at[0])
    c_dn = pltpu.make_async_copy(wdn, wd, wsem.at[1])
    c_q = [pltpu.make_async_copy(wqkv.at[:, pl.ds(QCHUNK * i, QCHUNK)], wq.at[i % QSLOTS], qsem.at[i]) for i in range(NQ)]

    def group(s):
        return target(s % 4) * 2 + (y + s // 4 + 1) % 2

    def c_kv(s):
        rows = pl.ds(8 * group(s), 8)
        return (pltpu.make_async_copy(kh.at[rows], ko.at[rows], ksem.at[s]),
                pltpu.make_async_copy(vh.at[rows], vo.at[rows], vsem.at[s]))

    def start_kv(s):
        for c in c_kv(s):
            c.start()

    c_o = [pltpu.make_async_copy(wout.at[pl.ds((2 * core + i) * FF, FF)], (wu, wd)[i], osem.at[i]) for i in range(2)]

    for c in c_in + [c_up, c_dn]:
        c.start()
    for i in range(3):
        c_q[i].start()

    barrier = pltpu.get_barrier_semaphore()
    pl.semaphore_signal(barrier, inc=1, device_id=partner, device_id_type=MESH)
    pl.semaphore_signal(barrier, inc=1, device_id=ypeer, device_id_type=MESH)
    for d in range(1, 4):
        pl.semaphore_signal(barrier, inc=1, device_id=zpeer(d), device_id_type=MESH)

    for c in c_in[:3]:
        c.wait()
    gamma = g_s[...].reshape(1, D)
    beta = b_s[...].reshape(1, D)

    def norm_rows(i, carry):
        rows = pl.ds(pl.multiple_of(16 * i, 16), 16)
        xf = x_s[rows, :].astype(F32)
        cen = xf - jnp.mean(xf, axis=-1, keepdims=True)
        var = jnp.mean(cen * cen, axis=-1, keepdims=True)
        h_s[rows, :] = (cen * lax.rsqrt(var + LN_EPS) * gamma + beta).astype(BF16)
        return carry

    lax.fori_loop(0, ROWS // 16, norm_rows, 0)

    for c in c_in[3:]:
        c.wait()
    for b in range(ROWS):
        posv[b:b + 1, :] = jnp.full((1, HD), pos[b], jnp.int32)
    angles = posv[...].astype(F32) * freq_s[...]
    cos = jnp.cos(angles)
    sin = jnp.sin(angles)
    sin = jnp.where(lax.broadcasted_iota(jnp.int32, (ROWS, HD), 1) < HD // 2, -sin, sin)

    c_up.wait()
    c_q[3].start()
    up = lax.dot_general(h_s[...], wu[...], (((1,), (1,)), ((), ())), preferred_element_type=F32)
    act[...] = (0.5 * up * (1.0 + lax.erf(up * (1.0 / math.sqrt(2.0))))).astype(BF16)
    c_dn.wait()

    def down(column_half, dst):
        cols = pl.ds(pl.multiple_of(HALF * HD * column_half, HD), HALF * HD)
        part = jnp.dot(act[...], wd[:, cols], preferred_element_type=F32)
        for j in range(HALF):
            dst[:, j] = part[:, HD * j:HD * (j + 1)].reshape(GROUPS, 8, HD)

    down(1 - core, ml.at[0])
    pl.semaphore_wait(barrier, 5)
    r_mld = remote(ml.at[0], mld, mld_s, mld_r, partner)
    r_mld.start()
    down(core, ml.at[1])


    def r_mly(j):
        return remote(mls.at[target(j), 1 - y], mly.at[j], mly_s.at[j], mly_r.at[j], ypeer)

    def r_mlz(j):
        return remote(mlz.at[j], mlr.at[slot(j)], mlz_s.at[j], mlz_r.at[slot(j)], target_dev(j))

    def mlp_z(j):
        r_mly(j).wait_recv()
        mlz[j] = mls[target(j), y] + mly[j]

    for ch in range(NQ):
        c_q[ch].wait()
        acc = jnp.dot(h_s[...], wq[ch % QSLOTS], preferred_element_type=F32).astype(BF16).astype(F32)
        if ch + QSLOTS < NQ:
            c_q[ch + QSLOTS].start()
        if ch >= 2:
            start_kv(ch - 2)
        for i in range(QCHUNK // HD):
            h = ch * (QCHUNK // HD) + i
            vec = acc[:, HD * i:HD * (i + 1)]
            if h <= NH:
                vec = rope(vec, cos, sin)
            vec = vec.reshape(GROUPS, 8, HD)
            if h < NH:
                q4[:, h] = vec
            elif h == NH:
                kn[...] = vec
            else:
                vn[...] = vec
        if ch == 1:
            r_mld.wait_recv()
            mls[...] = ml[1].reshape(4, 2, HALF, 8, HD) + mld[...].reshape(4, 2, HALF, 8, HD)
            for j in range(4):
                r_mly(j).start()

    col_id = lax.broadcasted_iota(jnp.int32, (NH, SEQ), 1)
    sub = lax.broadcasted_iota(jnp.int32, (NH, HD), 0)
    lane = lax.broadcasted_iota(jnp.int32, (NH, HD), 1)

    def attend(s):
        p = group(s)
        local = [pos[8 * p + r] - me * SEQ for r in range(8)]
        inside = [(x >= 0) & (x < SEQ) for x in local]
        qs = [q4[p, :, r, :] for r in range(8)]
        scores = [lax.dot_general(qs[r].astype(BF16), ko[8 * p + r], (((1,), (1,)), ((), ())), preferred_element_type=F32)
                  for r in range(8)]
        s_new = [jnp.sum(qs[r] * kn[p, r:r + 1, :], axis=-1, keepdims=True) * HD ** -0.5 for r in range(8)]
        s_new = [jnp.where(inside[r], s_new[r], NEG_FILL) for r in range(8)]
        masked = [jnp.where(col_id < local[r], scores[r] * HD ** -0.5, NEG_FILL) for r in range(8)]
        ms = [jnp.maximum(jnp.max(masked[r], axis=-1, keepdims=True), s_new[r]) for r in range(8)]
        es = [jnp.where(col_id < local[r], jnp.exp(masked[r] - ms[r]), 0.0) for r in range(8)]
        e_new = [jnp.where(inside[r], jnp.exp(s_new[r] - ms[r]), 0.0) for r in range(8)]
        os = [jnp.dot(es[r].astype(BF16), vo[8 * p + r], preferred_element_type=F32) for r in range(8)]
        ls = [jnp.sum(es[r], axis=-1, keepdims=True) + e_new[r] for r in range(8)]
        for r in range(8):
            o = os[r] + e_new[r].astype(BF16).astype(F32) * vn[p, r:r + 1, :]
            for half in range(2):
                idx = sub - HALF * half
                own = (idx >= 0) & (idx < HALF)
                t = jnp.where(own & (lane == idx), ms[r], jnp.where(own & (lane == idx + LANE_L), ls[r], 0.0))
                st[s, half, HALF, r:r + 1, :] = jnp.sum(t, axis=0, keepdims=True)
                st[s, half, 0:HALF, r, :] = o[HALF * half:HALF * (half + 1), :]

    def r_d2d(s):
        return remote(st.at[s, 1 - core], d2d.at[s], d2d_s.at[s], d2d_r.at[s], partner)

    def r_y(j):
        return remote(cmb.at[j], yrcv.at[j], sty_s.at[j], sty_r.at[j], ypeer)

    def r_z(j):
        return remote(zsnd.at[j], zrcv.at[slot(j)], stz_s.at[j], stz_r.at[slot(j)], target_dev(j))

    lane8 = lax.broadcasted_iota(jnp.int32, (8, HD), 1)

    def merge(dst, a, b):
        ta, tb = a[HALF], b[HALF]
        top = jnp.maximum(ta, tb)
        wa, wb = weights_of(ta, top), weights_of(tb, top)
        total = ta * pltpu.roll(wa, LANE_L, 1) + tb * pltpu.roll(wb, LANE_L, 1)
        dst[HALF] = jnp.where(lane8 < LANE_L, top, total)
        for i in range(HALF):
            dst[i] = a[i] * wa[:, i:i + 1] + b[i] * wb[:, i:i + 1]

    def pair(s):
        r_d2d(s).wait_recv()
        merge(cmb.at[s], st.at[s, core], d2d.at[s])

    def pair_y(j):
        r_y(j).wait_recv()
        merge(zsnd.at[j], cmb.at[4 + j], yrcv.at[j])

    def step(s, carry):
        ck, cv = c_kv(s)
        ck.wait()
        cv.wait()

        @pl.when(s < 4)
        def _():
            start_kv(s + 4)

        @pl.when(s == 4)
        def _():
            c_o[0].start()

        @pl.when(s == 5)
        def _():
            c_o[1].start()

        attend(s)
        r_d2d(s).start()

        @pl.when(s > 0)
        def _():
            pair(s - 1)

        @pl.when((s >= 1) & (s < 5))
        def _():
            r_y(s - 1).start()

        @pl.when((s >= 1) & (s < 4))
        def _():
            mlp_z(s - 1)
            r_mlz(s - 1).start()

        @pl.when(s >= 5)
        def _():
            pair_y(s - 5)
            r_z(s - 5).start()

        return carry

    lax.fori_loop(0, GROUPS, step, 0)
    mlp_z(3)
    pair(GROUPS - 1)
    pair_y(3)
    for j in range(3):
        r_z(j).wait_recv()
    parts = [zsnd.at[3], zrcv.at[0], zrcv.at[1], zrcv.at[2]]
    tiles = [part[HALF] for part in parts]
    top = functools.reduce(jnp.maximum, tiles)
    ws = [weights_of(t, top) for t in tiles]
    total = functools.reduce(jnp.add, [t * pltpu.roll(w, LANE_L, 1) for t, w in zip(tiles, ws)])
    heads = []
    for i in range(HALF):
        acc = functools.reduce(jnp.add, [part[i] * w[:, i:i + 1] for part, w in zip(parts, ws)])
        heads.append((acc / total[:, LANE_L + i:LANE_L + i + 1]).astype(BF16))
    ctx = jnp.concatenate(heads, axis=1)

    def project(column_half):
        cols = pl.ds(pl.multiple_of(HALF * HD * column_half, HD), HALF * HD)
        return (jnp.dot(ctx[:, :FF], wu[:, cols], preferred_element_type=F32)
                + jnp.dot(ctx[:, FF:], wd[:, cols], preferred_element_type=F32))

    c_o[0].wait()
    c_o[1].wait()
    other = project(1 - core)
    for i in range(HALF):
        wsend[i] = other[:, HD * i:HD * (i + 1)]
    r_wo = remote(wsend, wrecv, wo_s, wo_r, partner)
    r_wo.start()
    mine = project(core)
    for j in range(3):
        r_mlz(j).wait_recv()
    fin = mlz[3] + mlr[0] + mlr[1] + mlr[2]
    r_wo.wait_recv()
    for i in range(HALF):
        agb[chip, core, i] = mine[:, HD * i:HD * (i + 1)] + wrecv[i] + fin[i]

    def piece(zz, yy):
        return agb.at[zz * 2 + yy, core]

    def send_z(d):
        return remote(piece(z, y), piece(z, y), agz_s.at[d - 1], agz_r.at[d - 1], zpeer(d))

    def send_y(d):
        zz = (z + 4 - d) % 4
        return remote(piece(zz, y), piece(zz, y), agy_s.at[d], agy_r.at[d], ypeer)

    def send_c(d, other_y):
        zz = (z + 4 - d) % 4
        yy = (y + other_y) % 2
        return remote(piece(zz, yy), piece(zz, yy), agc_s.at[2 * d + other_y], agc_r.at[2 * d + other_y], partner)

    flip = z // 2
    near = z + flip * (3 - 2 * z)
    order = [src + flip * (3 - 2 * src) for src in (1 - near, 2, 3)]
    dist = [(z + 4 - src) % 4 for src in order]
    for i in (2, 1, 0):
        send_z((order[i] + 4 - z) % 4).start()
    send_y(0).start()
    send_c(0, 0).start()
    for d in dist:
        send_z(d).wait_recv()
        send_y(d).start()
        send_c(d, 0).start()
    for d in [0] + dist:
        send_y(d).wait_recv()
        send_c(d, 1).start()
    for d in range(4):
        for o in range(2):
            send_c(d, o).wait_recv()

    r_mld.wait_send()
    for s in range(GROUPS):
        r_d2d(s).wait_send()
    for j in range(4):
        r_mly(j).wait_send()
        r_y(j).wait_send()
    for j in range(3):
        r_mlz(j).wait_send()
        r_z(j).wait_send()
    r_wo.wait_send()
    for d in (1, 2, 3):
        send_z(d).wait_send()
    for d in range(4):
        send_y(d).wait_send()
        send_c(d, 0).wait_send()
        send_c(d, 1).wait_send()


def write_kernel(pos, ko, vo, kn, vn, agb, x_ref, out, k_out, v_out, kw, vw, out_ref, sem):
    me = lax.axis_index("sp")
    sub = lax.broadcasted_iota(jnp.int32, (16, HD), 0)
    copies = []
    for i in range(GROUPS):
        for r in range(8):
            b = 8 * i + r
            local = pos[b] - me * SEQ

            @pl.when((local >= 0) & (local < SEQ))
            def _():
                tile = pl.ds(pl.multiple_of(local // 16 * 16, 16), 16)
                here = sub == local % 16
                kw[b, tile, :] = jnp.where(here, kn[i, r:r + 1, :], ko[b, tile, :].astype(F32)).astype(BF16)
                vw[b, tile, :] = jnp.where(here, vn[i, r:r + 1, :], vo[b, tile, :].astype(F32)).astype(BF16)

        rows = pl.ds(8 * i, 8)
        copies.append(pltpu.make_async_copy(kw.at[rows], k_out.at[rows], sem.at[2 * i]))
        copies.append(pltpu.make_async_copy(vw.at[rows], v_out.at[rows], sem.at[2 * i + 1]))
        copies[-2].start()
        copies[-1].start()
    for q in range(GROUPS // 2):
        rows = slice(16 * q, 16 * (q + 1))
        for j in range(NH):
            cols = slice(HD * j, HD * (j + 1))
            both = agb[2 * q:2 * q + 2, j // HALF, j % HALF].reshape(16, HD)
            out_ref[rows, cols] = (x_ref[rows, cols].astype(F32) + both).astype(BF16)
    copies.append(pltpu.make_async_copy(out_ref, out, sem.at[2 * GROUPS]))
    copies[-1].start()
    for c in copies:
        c.wait()


def in_hbm(array):
    return pltpu.with_memory_space_constraint(array, pltpu.HBM)


def in_vmem(array):
    return pltpu.with_memory_space_constraint(array, pltpu.VMEM)


def device_step(hidden, ln_gamma, ln_beta, w_qkv, w_out, w_up, w_down, k_cache, v_cache, positions):
    pair_ids = np.arange(0, HD, 2, dtype=np.float64) / HD
    freq = jnp.asarray(np.tile(ROPE_BASE ** -pair_ids, 2)[None], F32)

    vmem = pl.BlockSpec(memory_space=pltpu.VMEM)
    hbm = pl.BlockSpec(memory_space=pltpu.HBM)
    dma = pltpu.SemaphoreType.DMA
    agb, k_blk, v_blk, k_row, v_row = pl.pallas_call(
        main_kernel,
        out_shape=(
            pltpu.VMEM((GROUPS, 2, HALF, 8, HD), F32),
            pltpu.VMEM(k_cache.shape, BF16),
            pltpu.VMEM(v_cache.shape, BF16),
            pltpu.VMEM((GROUPS, 8, HD), F32),
            pltpu.VMEM((GROUPS, 8, HD), F32),
        ),
        in_specs=[hbm] * 11,
        out_specs=(vmem,) * 5,
        scratch_shapes=[
            pltpu.SMEM((ROWS,), jnp.int32),
            pltpu.VMEM((ROWS, D), BF16),
            pltpu.VMEM((D,), F32),
            pltpu.VMEM((D,), F32),
            pltpu.VMEM((1, HD), F32),
            pltpu.VMEM((ROWS, HD), jnp.int32),
            pltpu.VMEM((QSLOTS, D, QCHUNK), BF16),
            pltpu.VMEM((FF, D), BF16),
            pltpu.VMEM((FF, D), BF16),
            pltpu.VMEM((ROWS, D), BF16),
            pltpu.VMEM((ROWS, FF), BF16),
            pltpu.VMEM((GROUPS, NH, 8, HD), F32),
            pltpu.VMEM((GROUPS, 2, HALF + 1, 8, HD), F32),
            pltpu.VMEM((GROUPS, HALF + 1, 8, HD), F32),
            pltpu.VMEM((GROUPS, HALF + 1, 8, HD), F32),
            pltpu.VMEM((4, HALF + 1, 8, HD), F32),
            pltpu.VMEM((4, HALF + 1, 8, HD), F32),
            pltpu.VMEM((3, HALF + 1, 8, HD), F32),
            pltpu.VMEM((2, GROUPS, HALF, 8, HD), F32),
            pltpu.VMEM((GROUPS, HALF, 8, HD), F32),
            pltpu.VMEM((4, 2, HALF, 8, HD), F32),
            pltpu.VMEM((4, HALF, 8, HD), F32),
            pltpu.VMEM((4, HALF, 8, HD), F32),
            pltpu.VMEM((3, HALF, 8, HD), F32),
            pltpu.VMEM((HALF, 8, HD), F32),
            pltpu.VMEM((HALF, 8, HD), F32),
            dma((5,)), dma((2,)), dma((NQ,)), dma((2,)), dma((GROUPS,)), dma((GROUPS,)),
            dma((GROUPS,)), dma((GROUPS,)), dma((4,)), dma((4,)), dma((3,)), dma((3,)),
            dma, dma, dma((4,)), dma((4,)), dma((3,)), dma((3,)), dma, dma,
            dma((3,)), dma((3,)), dma((4,)), dma((4,)), dma((8,)), dma((8,)),
        ],
        compiler_params=pltpu.CompilerParams(collective_id=0, has_side_effects=True, vmem_limit_bytes=32 * 2**20),
        name="layer",
    )(*[in_hbm(a) for a in (positions, hidden, ln_gamma, ln_beta, freq,
                               w_qkv, w_out, w_up.T, w_down, k_cache, v_cache)])

    out, k_new, v_new, _, _ = pl.pallas_call(
        write_kernel,
        out_shape=(
            jax.ShapeDtypeStruct(hidden.shape, BF16),
            jax.ShapeDtypeStruct(k_cache.shape, BF16),
            jax.ShapeDtypeStruct(v_cache.shape, BF16),
            pltpu.VMEM(k_cache.shape, BF16),
            pltpu.VMEM(v_cache.shape, BF16),
        ),
        in_specs=[pl.BlockSpec(memory_space=pltpu.SMEM)] + [vmem] * 6,
        out_specs=(hbm, hbm, hbm, vmem, vmem),
        scratch_shapes=[pltpu.VMEM((ROWS, D), BF16), dma((2 * GROUPS + 1,))],
        input_output_aliases={1: 3, 2: 4},
        compiler_params=pltpu.CompilerParams(vmem_limit_bytes=16 * 2**20),
        name="write",
    )(positions, *[in_vmem(a) for a in (k_blk, v_blk, k_row, v_row, agb)], hidden)
    return out, k_new, v_new


def solution(mesh):
    cache_spec = P('dp', 'sp', None)
    in_specs = (P('dp', None), P(None), P(None), P(None, None), P(None, None), P(None, 'sp'), P('sp', None), cache_spec, cache_spec, P('dp'))
    out_specs = (P('dp', None), cache_spec, cache_spec)
    return jax.shard_map(device_step, mesh=mesh, in_specs=in_specs, out_specs=out_specs, check_vma=False)
```

```python
import functools
import math

import jax
import jax.numpy as jnp
import numpy as np
from jax import lax
from jax.experimental import pallas as pl
from jax.experimental.pallas import tpu as pltpu
from jax.sharding import PartitionSpec as P

LN_EPS = 1e-5
ROPE_BASE = 10000.0
NEG_FILL = -1e30
MESH = pl.DeviceIdType.MESH

ROWS = 64
D = 2816
HD = 128
NH = 22
HALF = 11
FF = 704
SEQ = 512
GROUPS = 8
LANE_L = 64
QCHUNK = 512
NQ = 3
QHEADS = QCHUNK // HD
F32 = jnp.float32
BF16 = jnp.bfloat16


def rope(vec, cos, sin_signed):
    return (vec * cos + pltpu.roll(vec, HD // 2, 1) * sin_signed).astype(BF16).astype(F32)


def remote(src, dst, ssem, rsem, dev):
    return pltpu.make_async_remote_copy(src, dst, ssem, rsem, device_id=dev, device_id_type=MESH)


def weights_of(tile, top):
    return jnp.exp(tile - top)


def main_kernel(pos_h, x_h, g_h, b_h, freq_h, wqkv, wout, wup, wdn, kh, vh,
                agb, ko, vo, kn, vn,
                pos, x_s, g_s, b_s, freq_s, posv, wq, wu, wd, h_s, act, q4,
                st, d2d, cmb, yrcv, zsnd, zrcv, ml, mld, mls, mly, mlz, mlr, wsend, wrecv,
                isem, wsem, qsem, osem, ksem, vsem,
                d2d_s, d2d_r, sty_s, sty_r, stz_s, stz_r, mld_s, mld_r, mly_s, mly_r, mlz_s, mlz_r, wo_s, wo_r,
                agz_s, agz_r, agy_s, agy_r, agc_s, agc_r, rq_s, rq_r):
    dp = lax.axis_index("dp")
    me = lax.axis_index("sp")
    core = me % 2
    chip = me // 2
    y = chip % 2
    z = chip // 2
    partner = (dp, me + 1 - 2 * core)
    ypeer = (dp, me + 2 - 4 * y)

    def zpeer(d):
        return (dp, ((z + d) % 4) * 4 + y * 2 + core)

    sign = 1 - 2 * (z // 2)

    def target(j):
        return (z + 4 + sign * (j + 1)) % 4

    def target_dev(j):
        return (dp, target(j) * 4 + y * 2 + core)

    def slot(j):
        return 1 + sign * (1 - j)

    c_in = [pltpu.make_async_copy(src, dst, isem.at[i])
            for i, (src, dst) in enumerate(((x_h, x_s), (g_h, g_s), (b_h, b_s), (freq_h, freq_s), (pos_h, pos)))]
    c_up = pltpu.make_async_copy(wup, wu, wsem.at[0])
    c_dn = pltpu.make_async_copy(wdn, wd, wsem.at[1])
    c_q = [pltpu.make_async_copy(wqkv.at[:, pl.ds(QCHUNK * (NQ * core + i), QCHUNK)], wq.at[i], qsem.at[i]) for i in range(NQ)]

    def group(s):
        return target(s % 4) * 2 + (y + s // 4 + 1) % 2

    def c_kv(s):
        rows = pl.ds(8 * group(s), 8)
        return (pltpu.make_async_copy(kh.at[rows], ko.at[rows], ksem.at[s]),
                pltpu.make_async_copy(vh.at[rows], vo.at[rows], vsem.at[s]))

    def start_kv(s):
        for c in c_kv(s):
            c.start()

    c_o = [pltpu.make_async_copy(wout.at[pl.ds((2 * core + i) * FF, FF)], (wu, wd)[i], osem.at[i]) for i in range(2)]

    for c in c_in + [c_up, c_dn]:
        c.start()
    for c in c_q:
        c.start()

    barrier = pltpu.get_barrier_semaphore()
    pl.semaphore_signal(barrier, inc=1, device_id=partner, device_id_type=MESH)
    pl.semaphore_signal(barrier, inc=1, device_id=ypeer, device_id_type=MESH)
    for d in range(1, 4):
        pl.semaphore_signal(barrier, inc=1, device_id=zpeer(d), device_id_type=MESH)

    for c in c_in[:3]:
        c.wait()
    gamma = g_s[...].reshape(1, D)
    beta = b_s[...].reshape(1, D)

    def norm_rows(i, carry):
        rows = pl.ds(pl.multiple_of(16 * i, 16), 16)
        xf = x_s[rows, :].astype(F32)
        cen = xf - jnp.mean(xf, axis=-1, keepdims=True)
        var = jnp.mean(cen * cen, axis=-1, keepdims=True)
        h_s[rows, :] = (cen * lax.rsqrt(var + LN_EPS) * gamma + beta).astype(BF16)
        return carry

    lax.fori_loop(0, ROWS // 16, norm_rows, 0)

    for c in c_in[3:]:
        c.wait()
    for b in range(ROWS):
        posv[b:b + 1, :] = jnp.full((1, HD), pos[b], jnp.int32)
    angles = posv[...].astype(F32) * freq_s[...]
    cos = jnp.cos(angles)
    sin = jnp.sin(angles)
    sin = jnp.where(lax.broadcasted_iota(jnp.int32, (ROWS, HD), 1) < HD // 2, -sin, sin)

    c_up.wait()
    up = lax.dot_general(h_s[...], wu[...], (((1,), (1,)), ((), ())), preferred_element_type=F32)
    act[...] = (0.5 * up * (1.0 + lax.erf(up * (1.0 / math.sqrt(2.0))))).astype(BF16)
    c_dn.wait()

    def down(column_half, dst):
        cols = pl.ds(pl.multiple_of(HALF * HD * column_half, HD), HALF * HD)
        part = jnp.dot(act[...], wd[:, cols], preferred_element_type=F32)
        for j in range(HALF):
            dst[:, j] = part[:, HD * j:HD * (j + 1)].reshape(GROUPS, 8, HD)

    down(1 - core, ml.at[0])
    pl.semaphore_wait(barrier, 5)
    r_mld = remote(ml.at[0], mld, mld_s, mld_r, partner)
    r_mld.start()
    down(core, ml.at[1])


    def r_mly(j):
        return remote(mls.at[target(j), 1 - y], mly.at[j], mly_s.at[j], mly_r.at[j], ypeer)

    def r_mlz(j):
        return remote(mlz.at[j], mlr.at[slot(j)], mlz_s.at[j], mlz_r.at[slot(j)], target_dev(j))

    def mlp_z(j):
        r_mly(j).wait_recv()
        mlz[j] = mls[target(j), y] + mly[j]

    def r_q(i):
        own = q4.at[:, pl.ds(QHEADS * (NQ * core + i), QHEADS)]
        return remote(own, own, rq_s.at[i], rq_r.at[i], partner)

    start_kv(0)
    for i in range(NQ):
        c_q[i].wait()
        acc = jnp.dot(h_s[...], wq[i], preferred_element_type=F32).astype(BF16).astype(F32)
        start_kv(i + 1)
        for t in range(QHEADS):
            vec = acc[:, HD * t:HD * (t + 1)]
            turned = rope(vec, cos, sin)
            if i == NQ - 1 and t == QHEADS - 1:
                turned = jnp.where(core == 1, vec, turned)
            q4[:, QHEADS * (NQ * core + i) + t] = turned.reshape(GROUPS, 8, HD)
        r_q(i).start()
        if i == 1:
            r_mld.wait_recv()
            mls[...] = ml[1].reshape(4, 2, HALF, 8, HD) + mld[...].reshape(4, 2, HALF, 8, HD)
            for j in range(4):
                r_mly(j).start()
    for i in range(NQ):
        r_q(i).wait_recv()
    kn[...] = q4[:, NH]
    vn[...] = q4[:, NH + 1]

    col_id = lax.broadcasted_iota(jnp.int32, (NH, SEQ), 1)
    sub = lax.broadcasted_iota(jnp.int32, (NH, HD), 0)
    lane = lax.broadcasted_iota(jnp.int32, (NH, HD), 1)

    def attend(s):
        p = group(s)
        local = [pos[8 * p + r] - me * SEQ for r in range(8)]
        inside = [(x >= 0) & (x < SEQ) for x in local]
        qs = [q4[p, 0:NH, r, :] for r in range(8)]
        scores = [lax.dot_general(qs[r].astype(BF16), ko[8 * p + r], (((1,), (1,)), ((), ())), preferred_element_type=F32)
                  for r in range(8)]
        s_new = [jnp.sum(qs[r] * kn[p, r:r + 1, :], axis=-1, keepdims=True) * HD ** -0.5 for r in range(8)]
        s_new = [jnp.where(inside[r], s_new[r], NEG_FILL) for r in range(8)]
        masked = [jnp.where(col_id < local[r], scores[r] * HD ** -0.5, NEG_FILL) for r in range(8)]
        ms = [jnp.maximum(jnp.max(masked[r], axis=-1, keepdims=True), s_new[r]) for r in range(8)]
        es = [jnp.where(col_id < local[r], jnp.exp(masked[r] - ms[r]), 0.0) for r in range(8)]
        e_new = [jnp.where(inside[r], jnp.exp(s_new[r] - ms[r]), 0.0) for r in range(8)]
        os = [jnp.dot(es[r].astype(BF16), vo[8 * p + r], preferred_element_type=F32) for r in range(8)]
        ls = [jnp.sum(es[r], axis=-1, keepdims=True) + e_new[r] for r in range(8)]
        for r in range(8):
            o = os[r] + e_new[r].astype(BF16).astype(F32) * vn[p, r:r + 1, :]
            for half in range(2):
                idx = sub - HALF * half
                own = (idx >= 0) & (idx < HALF)
                t = jnp.where(own & (lane == idx), ms[r], jnp.where(own & (lane == idx + LANE_L), ls[r], 0.0))
                st[s, half, HALF, r:r + 1, :] = jnp.sum(t, axis=0, keepdims=True)
                st[s, half, 0:HALF, r, :] = o[HALF * half:HALF * (half + 1), :]

    def r_d2d(s):
        return remote(st.at[s, 1 - core], d2d.at[s], d2d_s.at[s], d2d_r.at[s], partner)

    def r_y(j):
        return remote(cmb.at[j], yrcv.at[j], sty_s.at[j], sty_r.at[j], ypeer)

    def r_z(j):
        return remote(zsnd.at[j], zrcv.at[slot(j)], stz_s.at[j], stz_r.at[slot(j)], target_dev(j))

    lane8 = lax.broadcasted_iota(jnp.int32, (8, HD), 1)

    def merge(dst, a, b):
        ta, tb = a[HALF], b[HALF]
        top = jnp.maximum(ta, tb)
        wa, wb = weights_of(ta, top), weights_of(tb, top)
        total = ta * pltpu.roll(wa, LANE_L, 1) + tb * pltpu.roll(wb, LANE_L, 1)
        dst[HALF] = jnp.where(lane8 < LANE_L, top, total)
        for i in range(HALF):
            dst[i] = a[i] * wa[:, i:i + 1] + b[i] * wb[:, i:i + 1]

    def pair(s):
        r_d2d(s).wait_recv()
        merge(cmb.at[s], st.at[s, core], d2d.at[s])

    def pair_y(j):
        r_y(j).wait_recv()
        merge(zsnd.at[j], cmb.at[4 + j], yrcv.at[j])

    def step(s, carry):
        ck, cv = c_kv(s)
        ck.wait()
        cv.wait()

        @pl.when(s < 4)
        def _():
            start_kv(s + 4)

        @pl.when(s == 4)
        def _():
            c_o[0].start()

        @pl.when(s == 5)
        def _():
            c_o[1].start()

        attend(s)
        r_d2d(s).start()

        @pl.when(s > 0)
        def _():
            pair(s - 1)

        @pl.when((s >= 1) & (s < 5))
        def _():
            r_y(s - 1).start()

        @pl.when((s >= 1) & (s < 4))
        def _():
            mlp_z(s - 1)
            r_mlz(s - 1).start()

        @pl.when(s >= 5)
        def _():
            pair_y(s - 5)
            r_z(s - 5).start()

        return carry

    lax.fori_loop(0, GROUPS, step, 0)
    mlp_z(3)
    pair(GROUPS - 1)
    pair_y(3)
    for j in range(3):
        r_z(j).wait_recv()
    parts = [zsnd.at[3], zrcv.at[0], zrcv.at[1], zrcv.at[2]]
    tiles = [part[HALF] for part in parts]
    top = functools.reduce(jnp.maximum, tiles)
    ws = [weights_of(t, top) for t in tiles]
    total = functools.reduce(jnp.add, [t * pltpu.roll(w, LANE_L, 1) for t, w in zip(tiles, ws)])
    heads = []
    for i in range(HALF):
        acc = functools.reduce(jnp.add, [part[i] * w[:, i:i + 1] for part, w in zip(parts, ws)])
        heads.append((acc / total[:, LANE_L + i:LANE_L + i + 1]).astype(BF16))
    ctx = jnp.concatenate(heads, axis=1)

    def project(column_half):
        cols = pl.ds(pl.multiple_of(HALF * HD * column_half, HD), HALF * HD)
        return (jnp.dot(ctx[:, :FF], wu[:, cols], preferred_element_type=F32)
                + jnp.dot(ctx[:, FF:], wd[:, cols], preferred_element_type=F32))

    c_o[0].wait()
    c_o[1].wait()
    other = project(1 - core)
    for i in range(HALF):
        wsend[i] = other[:, HD * i:HD * (i + 1)]
    r_wo = remote(wsend, wrecv, wo_s, wo_r, partner)
    r_wo.start()
    mine = project(core)
    for j in range(3):
        r_mlz(j).wait_recv()
    fin = mlz[3] + mlr[0] + mlr[1] + mlr[2]
    r_wo.wait_recv()
    for i in range(HALF):
        agb[chip, core, i] = mine[:, HD * i:HD * (i + 1)] + wrecv[i] + fin[i]

    def piece(zz, yy):
        return agb.at[zz * 2 + yy, core]

    def send_z(d):
        return remote(piece(z, y), piece(z, y), agz_s.at[d - 1], agz_r.at[d - 1], zpeer(d))

    def send_y(d):
        zz = (z + 4 - d) % 4
        return remote(piece(zz, y), piece(zz, y), agy_s.at[d], agy_r.at[d], ypeer)

    def send_c(d, other_y):
        zz = (z + 4 - d) % 4
        yy = (y + other_y) % 2
        return remote(piece(zz, yy), piece(zz, yy), agc_s.at[2 * d + other_y], agc_r.at[2 * d + other_y], partner)

    flip = z // 2
    near = z + flip * (3 - 2 * z)
    order = [src + flip * (3 - 2 * src) for src in (1 - near, 2, 3)]
    dist = [(z + 4 - src) % 4 for src in order]
    for i in (2, 1, 0):
        send_z((order[i] + 4 - z) % 4).start()
    send_y(0).start()
    send_c(0, 0).start()
    for d in dist:
        send_z(d).wait_recv()
        send_y(d).start()
        send_c(d, 0).start()
    for d in [0] + dist:
        send_y(d).wait_recv()
        send_c(d, 1).start()
    for d in range(4):
        for o in range(2):
            send_c(d, o).wait_recv()

    r_mld.wait_send()
    for i in range(NQ):
        r_q(i).wait_send()
    for s in range(GROUPS):
        r_d2d(s).wait_send()
    for j in range(4):
        r_mly(j).wait_send()
        r_y(j).wait_send()
    for j in range(3):
        r_mlz(j).wait_send()
        r_z(j).wait_send()
    r_wo.wait_send()
    for d in (1, 2, 3):
        send_z(d).wait_send()
    for d in range(4):
        send_y(d).wait_send()
        send_c(d, 0).wait_send()
        send_c(d, 1).wait_send()


def write_kernel(pos, ko, vo, kn, vn, agb, x_ref, out, k_out, v_out, kw, vw, out_ref, sem):
    me = lax.axis_index("sp")
    sub = lax.broadcasted_iota(jnp.int32, (16, HD), 0)
    copies = []
    for i in range(GROUPS):
        for r in range(8):
            b = 8 * i + r
            local = pos[b] - me * SEQ

            @pl.when((local >= 0) & (local < SEQ))
            def _():
                tile = pl.ds(pl.multiple_of(local // 16 * 16, 16), 16)
                here = sub == local % 16
                kw[b, tile, :] = jnp.where(here, kn[i, r:r + 1, :], ko[b, tile, :].astype(F32)).astype(BF16)
                vw[b, tile, :] = jnp.where(here, vn[i, r:r + 1, :], vo[b, tile, :].astype(F32)).astype(BF16)

        rows = pl.ds(8 * i, 8)
        copies.append(pltpu.make_async_copy(kw.at[rows], k_out.at[rows], sem.at[2 * i]))
        copies.append(pltpu.make_async_copy(vw.at[rows], v_out.at[rows], sem.at[2 * i + 1]))
        copies[-2].start()
        copies[-1].start()
    for q in range(GROUPS // 2):
        rows = slice(16 * q, 16 * (q + 1))
        for j in range(NH):
            cols = slice(HD * j, HD * (j + 1))
            both = agb[2 * q:2 * q + 2, j // HALF, j % HALF].reshape(16, HD)
            out_ref[rows, cols] = (x_ref[rows, cols].astype(F32) + both).astype(BF16)
    copies.append(pltpu.make_async_copy(out_ref, out, sem.at[2 * GROUPS]))
    copies[-1].start()
    for c in copies:
        c.wait()


def in_hbm(array):
    return pltpu.with_memory_space_constraint(array, pltpu.HBM)


def in_vmem(array):
    return pltpu.with_memory_space_constraint(array, pltpu.VMEM)


def device_step(hidden, ln_gamma, ln_beta, w_qkv, w_out, w_up, w_down, k_cache, v_cache, positions):
    pair_ids = np.arange(0, HD, 2, dtype=np.float64) / HD
    freq = jnp.asarray(np.tile(ROPE_BASE ** -pair_ids, 2)[None], F32)

    vmem = pl.BlockSpec(memory_space=pltpu.VMEM)
    hbm = pl.BlockSpec(memory_space=pltpu.HBM)
    dma = pltpu.SemaphoreType.DMA
    agb, k_blk, v_blk, k_row, v_row = pl.pallas_call(
        main_kernel,
        out_shape=(
            pltpu.VMEM((GROUPS, 2, HALF, 8, HD), F32),
            pltpu.VMEM(k_cache.shape, BF16),
            pltpu.VMEM(v_cache.shape, BF16),
            pltpu.VMEM((GROUPS, 8, HD), F32),
            pltpu.VMEM((GROUPS, 8, HD), F32),
        ),
        in_specs=[hbm] * 11,
        out_specs=(vmem,) * 5,
        scratch_shapes=[
            pltpu.SMEM((ROWS,), jnp.int32),
            pltpu.VMEM((ROWS, D), BF16),
            pltpu.VMEM((D,), F32),
            pltpu.VMEM((D,), F32),
            pltpu.VMEM((1, HD), F32),
            pltpu.VMEM((ROWS, HD), jnp.int32),
            pltpu.VMEM((NQ, D, QCHUNK), BF16),
            pltpu.VMEM((FF, D), BF16),
            pltpu.VMEM((FF, D), BF16),
            pltpu.VMEM((ROWS, D), BF16),
            pltpu.VMEM((ROWS, FF), BF16),
            pltpu.VMEM((GROUPS, NH + 2, 8, HD), F32),
            pltpu.VMEM((GROUPS, 2, HALF + 1, 8, HD), F32),
            pltpu.VMEM((GROUPS, HALF + 1, 8, HD), F32),
            pltpu.VMEM((GROUPS, HALF + 1, 8, HD), F32),
            pltpu.VMEM((4, HALF + 1, 8, HD), F32),
            pltpu.VMEM((4, HALF + 1, 8, HD), F32),
            pltpu.VMEM((3, HALF + 1, 8, HD), F32),
            pltpu.VMEM((2, GROUPS, HALF, 8, HD), F32),
            pltpu.VMEM((GROUPS, HALF, 8, HD), F32),
            pltpu.VMEM((4, 2, HALF, 8, HD), F32),
            pltpu.VMEM((4, HALF, 8, HD), F32),
            pltpu.VMEM((4, HALF, 8, HD), F32),
            pltpu.VMEM((3, HALF, 8, HD), F32),
            pltpu.VMEM((HALF, 8, HD), F32),
            pltpu.VMEM((HALF, 8, HD), F32),
            dma((5,)), dma((2,)), dma((NQ,)), dma((2,)), dma((GROUPS,)), dma((GROUPS,)),
            dma((GROUPS,)), dma((GROUPS,)), dma((4,)), dma((4,)), dma((3,)), dma((3,)),
            dma, dma, dma((4,)), dma((4,)), dma((3,)), dma((3,)), dma, dma,
            dma((3,)), dma((3,)), dma((4,)), dma((4,)), dma((8,)), dma((8,)), dma((NQ,)), dma((NQ,)),
        ],
        compiler_params=pltpu.CompilerParams(collective_id=0, has_side_effects=True, vmem_limit_bytes=32 * 2**20),
        name="layer",
    )(*[in_hbm(a) for a in (positions, hidden, ln_gamma, ln_beta, freq,
                               w_qkv, w_out, w_up.T, w_down, k_cache, v_cache)])

    out, k_new, v_new, _, _ = pl.pallas_call(
        write_kernel,
        out_shape=(
            jax.ShapeDtypeStruct(hidden.shape, BF16),
            jax.ShapeDtypeStruct(k_cache.shape, BF16),
            jax.ShapeDtypeStruct(v_cache.shape, BF16),
            pltpu.VMEM(k_cache.shape, BF16),
            pltpu.VMEM(v_cache.shape, BF16),
        ),
        in_specs=[pl.BlockSpec(memory_space=pltpu.SMEM)] + [vmem] * 6,
        out_specs=(hbm, hbm, hbm, vmem, vmem),
        scratch_shapes=[pltpu.VMEM((ROWS, D), BF16), dma((2 * GROUPS + 1,))],
        input_output_aliases={1: 3, 2: 4},
        compiler_params=pltpu.CompilerParams(vmem_limit_bytes=16 * 2**20),
        name="write",
    )(positions, *[in_vmem(a) for a in (k_blk, v_blk, k_row, v_row, agb)], hidden)
    return out, k_new, v_new


def solution(mesh):
    cache_spec = P('dp', 'sp', None)
    in_specs = (P('dp', None), P(None), P(None), P(None, None), P(None, None), P(None, 'sp'), P('sp', None), cache_spec, cache_spec, P('dp'))
    out_specs = (P('dp', None), cache_spec, cache_spec)
    return jax.shard_map(device_step, mesh=mesh, in_specs=in_specs, out_specs=out_specs, check_vma=False)
```

```python
import functools
import math

import jax
import jax.numpy as jnp
import numpy as np
from jax import lax
from jax.experimental import pallas as pl
from jax.experimental.pallas import tpu as pltpu
from jax.sharding import PartitionSpec as P

LN_EPS = 1e-5
ROPE_BASE = 10000.0
NEG_FILL = -1e30
MESH = pl.DeviceIdType.MESH

ROWS = 64
D = 2816
HD = 128
NH = 22
HALF = 11
FF = 704
SEQ = 512
GROUPS = 8
LANE_L = 64
QCHUNK = 512
NQ = 3
QHEADS = QCHUNK // HD
F32 = jnp.float32
BF16 = jnp.bfloat16


def rope(vec, cos, sin_signed):
    return (vec * cos + pltpu.roll(vec, HD // 2, 1) * sin_signed).astype(BF16).astype(F32)


def remote(src, dst, ssem, rsem, dev):
    return pltpu.make_async_remote_copy(src, dst, ssem, rsem, device_id=dev, device_id_type=MESH)


def weights_of(tile, top):
    return jnp.exp(tile - top)


def main_kernel(pos_h, x_h, g_h, b_h, freq_h, wqkv, wout, wup, wdn, kh, vh,
                agb, ko, vo, kn, vn,
                pos, x_s, g_s, b_s, freq_s, posv, wq, wu, wd, h_s, act, q4,
                st, d2d, cmb, yrcv, zsnd, zrcv, ml, mld, mls, mly, mlz, mlr, wsend, wrecv,
                isem, wsem, qsem, osem, ksem, vsem,
                d2d_s, d2d_r, sty_s, sty_r, stz_s, stz_r, mld_s, mld_r, mly_s, mly_r, mlz_s, mlz_r, wo_s, wo_r,
                agz_s, agz_r, agy_s, agy_r, agc_s, agc_r, rq_s, rq_r):
    dp = lax.axis_index("dp")
    me = lax.axis_index("sp")
    core = me % 2
    chip = me // 2
    y = chip % 2
    z = chip // 2
    partner = (dp, me + 1 - 2 * core)
    ypeer = (dp, me + 2 - 4 * y)

    def zpeer(d):
        return (dp, ((z + d) % 4) * 4 + y * 2 + core)

    sign = 1 - 2 * (z // 2)

    def target(j):
        return (z + 4 + sign * (j + 1)) % 4

    def target_dev(j):
        return (dp, target(j) * 4 + y * 2 + core)

    def slot(j):
        return 1 + sign * (1 - j)

    c_in = [pltpu.make_async_copy(src, dst, isem.at[i])
            for i, (src, dst) in enumerate(((x_h, x_s), (g_h, g_s), (b_h, b_s), (freq_h, freq_s), (pos_h, pos)))]
    c_up = pltpu.make_async_copy(wup, wu, wsem.at[0])
    c_dn = pltpu.make_async_copy(wdn, wd, wsem.at[1])
    c_q = [pltpu.make_async_copy(wqkv.at[:, pl.ds(QCHUNK * (NQ * core + i), QCHUNK)], wq.at[i], qsem.at[i]) for i in range(NQ)]

    def group(s):
        return target(s % 4) * 2 + (y + s // 4 + 1) % 2

    def c_kv(s):
        rows = pl.ds(8 * group(s), 8)
        return (pltpu.make_async_copy(kh.at[rows], ko.at[rows], ksem.at[s]),
                pltpu.make_async_copy(vh.at[rows], vo.at[rows], vsem.at[s]))

    def start_kv(s):
        for c in c_kv(s):
            c.start()

    c_o = [pltpu.make_async_copy(wout.at[pl.ds((2 * core + i) * FF, FF)], (wu, wd)[i], osem.at[i]) for i in range(2)]

    for c in c_in + [c_up, c_dn]:
        c.start()
    for c in c_q:
        c.start()

    barrier = pltpu.get_barrier_semaphore()
    pl.semaphore_signal(barrier, inc=1, device_id=partner, device_id_type=MESH)
    pl.semaphore_signal(barrier, inc=1, device_id=ypeer, device_id_type=MESH)
    for d in range(1, 4):
        pl.semaphore_signal(barrier, inc=1, device_id=zpeer(d), device_id_type=MESH)

    for c in c_in[:3]:
        c.wait()
    gamma = g_s[...].reshape(1, D)
    beta = b_s[...].reshape(1, D)

    def norm_rows(i, carry):
        rows = pl.ds(pl.multiple_of(16 * i, 16), 16)
        xf = x_s[rows, :].astype(F32)
        cen = xf - jnp.mean(xf, axis=-1, keepdims=True)
        var = jnp.mean(cen * cen, axis=-1, keepdims=True)
        h_s[rows, :] = (cen * lax.rsqrt(var + LN_EPS) * gamma + beta).astype(BF16)
        return carry

    lax.fori_loop(0, ROWS // 16, norm_rows, 0)

    for c in c_in[3:]:
        c.wait()
    for b in range(ROWS):
        posv[b:b + 1, :] = jnp.full((1, HD), pos[b], jnp.int32)
    angles = posv[...].astype(F32) * freq_s[...]
    cos = jnp.cos(angles)
    sin = jnp.sin(angles)
    sin = jnp.where(lax.broadcasted_iota(jnp.int32, (ROWS, HD), 1) < HD // 2, -sin, sin)

    c_up.wait()
    up = lax.dot_general(h_s[...], wu[...], (((1,), (1,)), ((), ())), preferred_element_type=F32)
    act[...] = (0.5 * up * (1.0 + lax.erf(up * (1.0 / math.sqrt(2.0))))).astype(BF16)
    c_dn.wait()

    def down(column_half, dst):
        cols = pl.ds(pl.multiple_of(HALF * HD * column_half, HD), HALF * HD)
        part = jnp.dot(act[...], wd[:, cols], preferred_element_type=F32)
        for j in range(HALF):
            dst[:, j] = part[:, HD * j:HD * (j + 1)].reshape(GROUPS, 8, HD)

    down(1 - core, ml.at[0])
    pl.semaphore_wait(barrier, 5)
    r_mld = remote(ml.at[0], mld, mld_s, mld_r, partner)
    r_mld.start()
    down(core, ml.at[1])


    def r_mly(j):
        return remote(mls.at[target(j), 1 - y], mly.at[j], mly_s.at[j], mly_r.at[j], ypeer)

    def r_mlz(j):
        return remote(mlz.at[j], mlr.at[slot(j)], mlz_s.at[j], mlz_r.at[slot(j)], target_dev(j))

    def mlp_z(j):
        r_mly(j).wait_recv()
        mlz[j] = mls[target(j), y] + mly[j]

    def r_q(i):
        own = q4.at[:, pl.ds(QHEADS * (NQ * core + i), QHEADS)]
        return remote(own, own, rq_s.at[i], rq_r.at[i], partner)

    start_kv(0)
    for i in range(NQ):
        c_q[i].wait()
        acc = jnp.dot(h_s[...], wq[i], preferred_element_type=F32).astype(BF16).astype(F32)
        start_kv(i + 1)
        for t in range(QHEADS):
            vec = acc[:, HD * t:HD * (t + 1)]
            turned = rope(vec, cos, sin)
            if i == NQ - 1 and t == QHEADS - 1:
                turned = jnp.where(core == 1, vec, turned)
            q4[:, QHEADS * (NQ * core + i) + t] = turned.reshape(GROUPS, 8, HD)
        r_q(i).start()
        if i == 1:
            r_mld.wait_recv()
            mls[...] = ml[1].reshape(4, 2, HALF, 8, HD) + mld[...].reshape(4, 2, HALF, 8, HD)
            for j in range(4):
                r_mly(j).start()
    for i in range(NQ):
        r_q(i).wait_recv()
    kn[...] = q4[:, NH]
    vn[...] = q4[:, NH + 1]

    col_id = lax.broadcasted_iota(jnp.int32, (NH, SEQ), 1)
    sub = lax.broadcasted_iota(jnp.int32, (NH, HD), 0)
    lane = lax.broadcasted_iota(jnp.int32, (NH, HD), 1)

    def attend(s):
        p = group(s)
        local = [pos[8 * p + r] - me * SEQ for r in range(8)]
        inside = [(x >= 0) & (x < SEQ) for x in local]
        qs = [q4[p, 0:NH, r, :] for r in range(8)]
        scores = [lax.dot_general(qs[r].astype(BF16), ko[8 * p + r], (((1,), (1,)), ((), ())), preferred_element_type=F32)
                  for r in range(8)]
        s_new = [jnp.sum(qs[r] * kn[p, r:r + 1, :], axis=-1, keepdims=True) * HD ** -0.5 for r in range(8)]
        s_new = [jnp.where(inside[r], s_new[r], NEG_FILL) for r in range(8)]
        masked = [jnp.where(col_id < local[r], scores[r] * HD ** -0.5, NEG_FILL) for r in range(8)]
        ms = [jnp.maximum(jnp.max(masked[r], axis=-1, keepdims=True), s_new[r]) for r in range(8)]
        es = [jnp.where(col_id < local[r], jnp.exp(masked[r] - ms[r]), 0.0) for r in range(8)]
        e_new = [jnp.where(inside[r], jnp.exp(s_new[r] - ms[r]), 0.0) for r in range(8)]
        os = [jnp.dot(es[r].astype(BF16), vo[8 * p + r], preferred_element_type=F32) for r in range(8)]
        ls = [jnp.sum(es[r], axis=-1, keepdims=True) + e_new[r] for r in range(8)]
        for r in range(8):
            o = os[r] + e_new[r].astype(BF16).astype(F32) * vn[p, r:r + 1, :]
            for half in range(2):
                idx = sub - HALF * half
                own = (idx >= 0) & (idx < HALF)
                t = jnp.where(own & (lane == idx), ms[r], jnp.where(own & (lane == idx + LANE_L), ls[r], 0.0))
                st[s, half, HALF, r:r + 1, :] = jnp.sum(t, axis=0, keepdims=True)
                st[s, half, 0:HALF, r, :] = o[HALF * half:HALF * (half + 1), :]

    def r_d2d(s):
        return remote(st.at[s, 1 - core], d2d.at[s], d2d_s.at[s], d2d_r.at[s], partner)

    def r_y(j):
        return remote(cmb.at[j], yrcv.at[j], sty_s.at[j], sty_r.at[j], ypeer)

    def r_z(j):
        return remote(zsnd.at[j], zrcv.at[slot(j)], stz_s.at[j], stz_r.at[slot(j)], target_dev(j))

    lane8 = lax.broadcasted_iota(jnp.int32, (8, HD), 1)

    def merge(dst, a, b):
        ta, tb = a[HALF], b[HALF]
        top = jnp.maximum(ta, tb)
        wa, wb = weights_of(ta, top), weights_of(tb, top)
        total = ta * pltpu.roll(wa, LANE_L, 1) + tb * pltpu.roll(wb, LANE_L, 1)
        dst[HALF] = jnp.where(lane8 < LANE_L, top, total)
        for i in range(HALF):
            dst[i] = a[i] * wa[:, i:i + 1] + b[i] * wb[:, i:i + 1]

    def pair(s):
        r_d2d(s).wait_recv()
        merge(cmb.at[s], st.at[s, core], d2d.at[s])

    def pair_y(j):
        r_y(j).wait_recv()
        merge(zsnd.at[j], cmb.at[4 + j], yrcv.at[j])

    def step(s, carry):
        ck, cv = c_kv(s)
        ck.wait()
        cv.wait()

        @pl.when(s < 4)
        def _():
            start_kv(s + 4)

        @pl.when(s == 4)
        def _():
            c_o[0].start()

        @pl.when(s == 5)
        def _():
            c_o[1].start()

        attend(s)
        r_d2d(s).start()

        @pl.when(s > 0)
        def _():
            pair(s - 1)

        @pl.when((s >= 1) & (s < 5))
        def _():
            r_y(s - 1).start()

        @pl.when((s >= 1) & (s < 4))
        def _():
            mlp_z(s - 1)
            r_mlz(s - 1).start()

        @pl.when(s >= 5)
        def _():
            pair_y(s - 5)
            r_z(s - 5).start()

        return carry

    lax.fori_loop(0, GROUPS, step, 0)
    mlp_z(3)
    pair(GROUPS - 1)
    pair_y(3)
    for j in range(3):
        r_z(j).wait_recv()
    parts = [zsnd.at[3], zrcv.at[0], zrcv.at[1], zrcv.at[2]]
    tiles = [part[HALF] for part in parts]
    top = functools.reduce(jnp.maximum, tiles)
    ws = [weights_of(t, top) for t in tiles]
    total = functools.reduce(jnp.add, [t * pltpu.roll(w, LANE_L, 1) for t, w in zip(tiles, ws)])
    heads = []
    for i in range(HALF):
        acc = functools.reduce(jnp.add, [part[i] * w[:, i:i + 1] for part, w in zip(parts, ws)])
        heads.append((acc / total[:, LANE_L + i:LANE_L + i + 1]).astype(BF16))
    ctx = jnp.concatenate(heads, axis=1)

    def project(column_half):
        cols = pl.ds(pl.multiple_of(HALF * HD * column_half, HD), HALF * HD)
        return (jnp.dot(ctx[:, :FF], wu[:, cols], preferred_element_type=F32)
                + jnp.dot(ctx[:, FF:], wd[:, cols], preferred_element_type=F32))

    c_o[0].wait()
    c_o[1].wait()
    other = project(1 - core)
    for i in range(HALF):
        wsend[i] = other[:, HD * i:HD * (i + 1)]
    r_wo = remote(wsend, wrecv, wo_s, wo_r, partner)
    r_wo.start()
    mine = project(core)
    for j in range(3):
        r_mlz(j).wait_recv()
    fin = mlz[3] + mlr[0] + mlr[1] + mlr[2]
    r_wo.wait_recv()
    for i in range(HALF):
        agb[chip, core, i] = mine[:, HD * i:HD * (i + 1)] + wrecv[i] + fin[i]

    def piece(zz, yy):
        return agb.at[zz * 2 + yy, core]

    def send_z(d):
        return remote(piece(z, y), piece(z, y), agz_s.at[d - 1], agz_r.at[d - 1], zpeer(d))

    def send_y(d):
        zz = (z + 4 - d) % 4
        return remote(piece(zz, y), piece(zz, y), agy_s.at[d], agy_r.at[d], ypeer)

    def send_c(d, other_y):
        zz = (z + 4 - d) % 4
        yy = (y + other_y) % 2
        return remote(piece(zz, yy), piece(zz, yy), agc_s.at[2 * d + other_y], agc_r.at[2 * d + other_y], partner)

    flip = z // 2
    near = z + flip * (3 - 2 * z)
    order = [src + flip * (3 - 2 * src) for src in (1 - near, 2, 3)]
    dist = [(z + 4 - src) % 4 for src in order]
    for i in (2, 1, 0):
        send_z((order[i] + 4 - z) % 4).start()
    send_y(0).start()
    send_c(0, 0).start()
    for d in dist:
        send_z(d).wait_recv()
        send_y(d).start()
        send_c(d, 0).start()
    for d in [0] + dist:
        send_y(d).wait_recv()
        send_c(d, 1).start()
    for d in range(4):
        for o in range(2):
            send_c(d, o).wait_recv()

    r_mld.wait_send()
    for i in range(NQ):
        r_q(i).wait_send()
    for s in range(GROUPS):
        r_d2d(s).wait_send()
    for j in range(4):
        r_mly(j).wait_send()
        r_y(j).wait_send()
    for j in range(3):
        r_mlz(j).wait_send()
        r_z(j).wait_send()
    r_wo.wait_send()
    for d in (1, 2, 3):
        send_z(d).wait_send()
    for d in range(4):
        send_y(d).wait_send()
        send_c(d, 0).wait_send()
        send_c(d, 1).wait_send()


def write_kernel(pos, ko, vo, kn, vn, agb, x_ref, out, k_out, v_out, kw, vw, out_ref, sem):
    me = lax.axis_index("sp")
    sub = lax.broadcasted_iota(jnp.int32, (16, HD), 0)
    copies = []
    for i in range(GROUPS):
        for r in range(8):
            b = 8 * i + r
            local = pos[b] - me * SEQ

            @pl.when((local >= 0) & (local < SEQ))
            def _():
                tile = pl.ds(pl.multiple_of(local // 16 * 16, 16), 16)
                here = sub == local % 16
                kw[b, tile, :] = jnp.where(here, kn[i, r:r + 1, :], ko[b, tile, :].astype(F32)).astype(BF16)
                vw[b, tile, :] = jnp.where(here, vn[i, r:r + 1, :], vo[b, tile, :].astype(F32)).astype(BF16)

            if r % 4 == 3:
                part = 2 * i + r // 4
                rows = pl.ds(4 * part, 4)
                copies.append(pltpu.make_async_copy(kw.at[rows], k_out.at[rows], sem.at[2 * part]))
                copies.append(pltpu.make_async_copy(vw.at[rows], v_out.at[rows], sem.at[2 * part + 1]))
                copies[-2].start()
                copies[-1].start()
    for q in range(GROUPS // 2):
        rows = slice(16 * q, 16 * (q + 1))
        for j in range(NH):
            cols = slice(HD * j, HD * (j + 1))
            both = agb[2 * q:2 * q + 2, j // HALF, j % HALF].reshape(16, HD)
            out_ref[rows, cols] = (x_ref[rows, cols].astype(F32) + both).astype(BF16)
    copies.append(pltpu.make_async_copy(out_ref, out, sem.at[4 * GROUPS]))
    copies[-1].start()
    for c in copies:
        c.wait()


def in_hbm(array):
    return pltpu.with_memory_space_constraint(array, pltpu.HBM)


def in_vmem(array):
    return pltpu.with_memory_space_constraint(array, pltpu.VMEM)


def device_step(hidden, ln_gamma, ln_beta, w_qkv, w_out, w_up, w_down, k_cache, v_cache, positions):
    pair_ids = np.arange(0, HD, 2, dtype=np.float64) / HD
    freq = jnp.asarray(np.tile(ROPE_BASE ** -pair_ids, 2)[None], F32)

    vmem = pl.BlockSpec(memory_space=pltpu.VMEM)
    hbm = pl.BlockSpec(memory_space=pltpu.HBM)
    dma = pltpu.SemaphoreType.DMA
    agb, k_blk, v_blk, k_row, v_row = pl.pallas_call(
        main_kernel,
        out_shape=(
            pltpu.VMEM((GROUPS, 2, HALF, 8, HD), F32),
            pltpu.VMEM(k_cache.shape, BF16),
            pltpu.VMEM(v_cache.shape, BF16),
            pltpu.VMEM((GROUPS, 8, HD), F32),
            pltpu.VMEM((GROUPS, 8, HD), F32),
        ),
        in_specs=[hbm] * 11,
        out_specs=(vmem,) * 5,
        scratch_shapes=[
            pltpu.SMEM((ROWS,), jnp.int32),
            pltpu.VMEM((ROWS, D), BF16),
            pltpu.VMEM((D,), F32),
            pltpu.VMEM((D,), F32),
            pltpu.VMEM((1, HD), F32),
            pltpu.VMEM((ROWS, HD), jnp.int32),
            pltpu.VMEM((NQ, D, QCHUNK), BF16),
            pltpu.VMEM((FF, D), BF16),
            pltpu.VMEM((FF, D), BF16),
            pltpu.VMEM((ROWS, D), BF16),
            pltpu.VMEM((ROWS, FF), BF16),
            pltpu.VMEM((GROUPS, NH + 2, 8, HD), F32),
            pltpu.VMEM((GROUPS, 2, HALF + 1, 8, HD), F32),
            pltpu.VMEM((GROUPS, HALF + 1, 8, HD), F32),
            pltpu.VMEM((GROUPS, HALF + 1, 8, HD), F32),
            pltpu.VMEM((4, HALF + 1, 8, HD), F32),
            pltpu.VMEM((4, HALF + 1, 8, HD), F32),
            pltpu.VMEM((3, HALF + 1, 8, HD), F32),
            pltpu.VMEM((2, GROUPS, HALF, 8, HD), F32),
            pltpu.VMEM((GROUPS, HALF, 8, HD), F32),
            pltpu.VMEM((4, 2, HALF, 8, HD), F32),
            pltpu.VMEM((4, HALF, 8, HD), F32),
            pltpu.VMEM((4, HALF, 8, HD), F32),
            pltpu.VMEM((3, HALF, 8, HD), F32),
            pltpu.VMEM((HALF, 8, HD), F32),
            pltpu.VMEM((HALF, 8, HD), F32),
            dma((5,)), dma((2,)), dma((NQ,)), dma((2,)), dma((GROUPS,)), dma((GROUPS,)),
            dma((GROUPS,)), dma((GROUPS,)), dma((4,)), dma((4,)), dma((3,)), dma((3,)),
            dma, dma, dma((4,)), dma((4,)), dma((3,)), dma((3,)), dma, dma,
            dma((3,)), dma((3,)), dma((4,)), dma((4,)), dma((8,)), dma((8,)), dma((NQ,)), dma((NQ,)),
        ],
        compiler_params=pltpu.CompilerParams(collective_id=0, has_side_effects=True, vmem_limit_bytes=32 * 2**20),
        name="layer",
    )(*[in_hbm(a) for a in (positions, hidden, ln_gamma, ln_beta, freq,
                               w_qkv, w_out, w_up.T, w_down, k_cache, v_cache)])

    out, k_new, v_new, _, _ = pl.pallas_call(
        write_kernel,
        out_shape=(
            jax.ShapeDtypeStruct(hidden.shape, BF16),
            jax.ShapeDtypeStruct(k_cache.shape, BF16),
            jax.ShapeDtypeStruct(v_cache.shape, BF16),
            pltpu.VMEM(k_cache.shape, BF16),
            pltpu.VMEM(v_cache.shape, BF16),
        ),
        in_specs=[pl.BlockSpec(memory_space=pltpu.SMEM)] + [vmem] * 6,
        out_specs=(hbm, hbm, hbm, vmem, vmem),
        scratch_shapes=[pltpu.VMEM((ROWS, D), BF16), dma((4 * GROUPS + 1,))],
        input_output_aliases={1: 3, 2: 4},
        compiler_params=pltpu.CompilerParams(vmem_limit_bytes=16 * 2**20),
        name="write",
    )(positions, *[in_vmem(a) for a in (k_blk, v_blk, k_row, v_row, agb)], hidden)
    return out, k_new, v_new


def solution(mesh):
    cache_spec = P('dp', 'sp', None)
    in_specs = (P('dp', None), P(None), P(None), P(None, None), P(None, None), P(None, 'sp'), P('sp', None), cache_spec, cache_spec, P('dp'))
    out_specs = (P('dp', None), cache_spec, cache_spec)
    return jax.shard_map(device_step, mesh=mesh, in_specs=in_specs, out_specs=out_specs, check_vma=False)
```
